32 devices in a mesh: group: 4 (over y, core), row: 2 (over x), col: 4 (over z).
Axes of the slice: x: 2, y: 2, z: 4, core: 2. Of those that a mesh axis runs over, the one named last changes fastest.
Arguments:
- fronts: bfloat16 [8, 12288, 12288], P('group', 'row', 'col'), may hold values from -0.0546875 to 0.0546875
- samples: bfloat16 [256, 8, 12288], P('row', 'group', 'col'), may hold values from -6 to 6
- second_samples: bfloat16 [256, 8, 12288], P('col', 'group', 'row'), may hold values from -6 to 6
- front_sizes: int32 [8], replicated, may hold values from 1536 to 12288, as said below
- parent_ids: int32 [8], replicated, may hold values from 1 to 8, as said below
- block_maps: int32 [8, 2], replicated, may hold values from 0 to 2, as said below
Outputs:
- sampled: bfloat16 [256, 8, 12288], P('col', 'group', 'row')
- projected: bfloat16 [256, 8, 12288], P('row', 'group', 'col')
The draws below stay inside these ranges and needn't reach their ends.
Inputs may be any that keep to these rules, and one draw needn't show every extreme that they name: `front_sizes`: every front has at least 1536 rows and some front has exactly 12288. `parent_ids`: a front's parent has a larger index; 8 marks a root; the last front is a root. `block_maps`: for a front f with a parent p, entry b with b * 6144 < front_sizes[f] names a parent block q with q * 6144 < front_sizes[p]; all other entries are 2; several child blocks may name one parent block.
All inputs are finite; a program needn't handle non-finite values.
Results may differ from the reference program's by a relative error of at most 0.009.
Values may be sent and summed in bfloat16 or wider, within the bound.
A program may use at most 192 MiB of HBM per device.

```python
import jax
import jax.numpy as jnp
from jax import lax

M = 12288
S = 256
FRONTS = 8
NB = 2
BLK = 6144


def tree_draw(key):
    base = jax.random.fold_in(key, 7)
    key_sizes, key_top, key_parent, key_blocks = jax.random.split(base, 4)
    indices = jnp.arange(FRONTS, dtype=jnp.int32)
    sizes = jax.random.randint(key_sizes, (FRONTS,), M // 8, M + 1, dtype=jnp.int32)
    largest = jax.random.randint(key_top, (), 0, FRONTS, dtype=jnp.int32)
    sizes = jnp.where(indices == largest, M, sizes)
    parents = jax.random.randint(key_parent, (FRONTS,), indices + 1, FRONTS + 1, dtype=jnp.int32)
    valid = (sizes + BLK - 1) // BLK
    parent_valid = valid[jnp.minimum(parents, FRONTS - 1)]
    targets = jax.random.randint(key_blocks, (FRONTS, NB), 0, parent_valid[:, None], dtype=jnp.int32)
    live = (jnp.arange(NB, dtype=jnp.int32)[None, :] < valid[:, None]) & (parents[:, None] < FRONTS)
    maps = jnp.where(live, targets, NB).astype(jnp.int32)
    return (sizes, parents, maps)


def draw_front_sizes(key, part):
    return tree_draw(key)[0]


def draw_parent_ids(key, part):
    return tree_draw(key)[1]


def draw_block_maps(key, part):
    return tree_draw(key)[2]


def block_levels(rng, extent, shards, least, top_value):
    def one(axis_at, shards_of):
        steps = jax.random.uniform(jax.random.fold_in(jax.random.fold_in(rng, 6), axis_at), (shards_of,), jnp.float32, least / len(shards), top_value / len(shards))
        return jnp.repeat(jnp.exp(steps), extent[axis_at] // shards_of).reshape((-1,) + (1,) * (len(extent) - axis_at - 1))

    gain = one(*shards[0])
    for cut in shards[1:]:
        gain = gain * one(*cut)
    return gain


def normal_values(own_key, dims, spread, reach, cuts=(), kind=jnp.bfloat16):
    array = spread * jax.random.normal(own_key, dims, jnp.float32)
    if cuts:
        array = array * block_levels(own_key, dims, cuts, -0.22, 0.18)
    return jnp.clip(array, -reach, reach).astype(kind)


def setup_inputs(seed: int = 0) -> dict:
    streams_of = jax.random.split(jax.random.key(seed), 7)
    fronts = normal_values(streams_of[0], (FRONTS, M, M), M ** -0.5, 0.0546875, ((0, 4), (1, 2), (2, 4)))
    samples = normal_values(streams_of[1], (S, FRONTS, M), 1.0, 6.0, ((0, 2), (1, 4), (2, 4)))
    second_samples = normal_values(streams_of[2], (S, FRONTS, M), 1.0, 6.0, ((0, 4), (1, 4), (2, 2)))
    front_sizes = draw_front_sizes(jax.random.fold_in(streams_of[6], 71), 0)
    parent_ids = draw_parent_ids(jax.random.fold_in(streams_of[6], 71), 0)
    block_maps = draw_block_maps(jax.random.fold_in(streams_of[6], 71), 0)
    return dict(fronts=fronts, samples=samples, second_samples=second_samples, front_sizes=front_sizes, parent_ids=parent_ids, block_maps=block_maps)


def reference(fronts, samples, second_samples, front_sizes, parent_ids, block_maps):
    positions = jnp.arange(M, dtype=jnp.int32)
    first_rows = []
    for front_index in range(FRONTS):
        keep_mask = (positions < front_sizes[front_index]).astype(jnp.float32)
        front_wide = fronts[front_index].astype(jnp.float32)
        chosen = samples[:, front_index, :].astype(jnp.float32) * keep_mask[None, :]
        product = jnp.einsum('sk,mk->sm', chosen, front_wide, precision=lax.Precision.HIGHEST)
        first_rows.append(product * keep_mask[None, :])
    sampled = jnp.stack(first_rows, axis=1).astype(jnp.bfloat16)
    parent_hot = (parent_ids[:, None] == jnp.arange(FRONTS, dtype=jnp.int32)[None, :]).astype(jnp.float32)
    block_hot = (block_maps[:, :, None] == jnp.arange(NB, dtype=jnp.int32)[None, None, :]).astype(jnp.float32)
    routing = jnp.einsum('fp,fbq->fpbq', parent_hot, block_hot)
    blocked = sampled.astype(jnp.float32).reshape(S, FRONTS, NB, BLK)
    extension = jnp.einsum('fpbq,sfbk->spqk', routing, blocked, precision=lax.Precision.HIGHEST)
    extension = extension.reshape(S, FRONTS, M)
    combined = (second_samples.astype(jnp.float32) + extension).astype(jnp.bfloat16)
    second_rows = []
    for front_index in range(FRONTS):
        keep_mask = (positions < front_sizes[front_index]).astype(jnp.float32)
        front_wide = fronts[front_index].astype(jnp.float32)
        chosen = combined[:, front_index, :].astype(jnp.float32) * keep_mask[None, :]
        product = jnp.dot(chosen, front_wide, precision=lax.Precision.HIGHEST)
        second_rows.append(product * keep_mask[None, :])
    projected = jnp.stack(second_rows, axis=1).astype(jnp.bfloat16)
    return sampled, projected
```

```python
import functools

import jax
import jax.numpy as jnp
from jax import lax
from jax.experimental import pallas as pl
from jax.experimental.pallas import tpu as pltpu
from jax.sharding import PartitionSpec as P

PASSES = 2
TILE = 256
SLOTS = 6
GATHER_SLOTS = 8
PARTIAL_SLOTS = 4
DRAIN = 2
SECOND_LAG = 9
FRONT_SLOTS = SECOND_LAG + 2


def swap_pairs(count):
    return [(0, 1), (1, 0)] if count == 2 else None


def gather_row(value, count, own_row, axis):
    if count != 2:
        return lax.all_gather(value, "row", axis=axis, tiled=True)
    other = lax.ppermute(value, "row", swap_pairs(count))
    first = own_row == 0
    return jnp.concatenate(
        [jnp.where(first, value, other), jnp.where(first, other, value)], axis=axis
    )


def scatter_row(value, count, own_row):
    if count != 2:
        return lax.psum_scatter(
            value.astype(jnp.bfloat16), "row", scatter_dimension=0, tiled=True
        ).astype(jnp.float32)
    half = value.shape[0] // 2
    kept = lax.dynamic_slice_in_dim(value, own_row * half, half, 0)
    sent = lax.dynamic_slice_in_dim(value, (1 - own_row) * half, half, 0).astype(jnp.bfloat16)
    return kept + lax.ppermute(sent, "row", swap_pairs(count)).astype(jnp.float32)


def shards(fronts, samples, second_samples, front_sizes, parent_ids, block_maps):
    local_count, tile_rows, tile_cols = fronts.shape
    row_count = lax.axis_size("row")
    own_group = lax.axis_index("group")
    own_row = lax.axis_index("row")
    own_col = lax.axis_index("col")
    total_fronts = parent_ids.shape[0]
    block_count = block_maps.shape[1]
    own_sizes = lax.dynamic_slice_in_dim(front_sizes, own_group * local_count, local_count, 0)
    row_keep = (own_row * tile_rows + jnp.arange(tile_rows, dtype=jnp.int32))[None, :] < own_sizes[
        :, None
    ]
    col_keep = (own_col * tile_cols + jnp.arange(tile_cols, dtype=jnp.int32))[None, :] < own_sizes[
        :, None
    ]
    own_fronts = own_group * local_count + jnp.arange(local_count, dtype=jnp.int32)
    masked = gather_row(samples, row_count, own_row, 0) * col_keep[None].astype(jnp.bfloat16)
    partial_value = jnp.einsum("sfk,fmk->sfm", masked, fronts, preferred_element_type=jnp.float32)
    partial_value = (partial_value * row_keep[None].astype(jnp.float32)).astype(jnp.bfloat16)
    sampled = lax.psum_scatter(partial_value, "col", scatter_dimension=0, tiled=True)
    portion = lax.all_gather(sampled, ("group", "row"), axis=1, tiled=True)
    number = portion.shape[1]
    source = jnp.arange(number, dtype=jnp.int32)
    front_index = source // (local_count * row_count) * local_count + source % local_count
    block_index = source // local_count % row_count
    front_hot = (front_index[:, None] == jnp.arange(total_fronts, dtype=jnp.int32)[None, :]).astype(
        jnp.int32
    )
    parent = jnp.sum(front_hot * parent_ids[None, :], axis=1)
    map_rows = jnp.sum(front_hot[:, :, None] * block_maps[None, :, :], axis=1)
    block_hot = (jnp.arange(block_count, dtype=jnp.int32)[None, :] == block_index[:, None]).astype(
        jnp.int32
    )
    target = jnp.sum(block_hot * map_rows, axis=1)
    weight = (parent[:, None] == own_fronts[None, :]) & (target[:, None] == own_row)
    extension = jnp.einsum(
        "sik,ij->sjk", portion, weight.astype(jnp.bfloat16), preferred_element_type=jnp.float32
    )
    combined = (second_samples.astype(jnp.float32) + extension).astype(jnp.bfloat16)
    combined = combined * row_keep[None].astype(jnp.bfloat16)
    gathered = lax.all_gather(combined, "col", axis=0, tiled=True)
    product = jnp.einsum("sfm,fmk->sfk", gathered, fronts, preferred_element_type=jnp.float32)
    projected = scatter_row(product, row_count, own_row)
    projected = (projected * col_keep[None].astype(jnp.float32)).astype(jnp.bfloat16)
    return (sampled, projected)


def remote(source, target, send_sem, recv_sem, device):
    return pltpu.make_async_remote_copy(
        src_ref=source,
        dst_ref=target,
        send_sem=send_sem,
        recv_sem=recv_sem,
        device_id=device,
        device_id_type=pl.DeviceIdType.MESH,
    )


def fused(
    cols,
    groups,
    samples,
    fronts,
    second,
    keep,
    from_blocks,
    to_parents,
    sampled,
    projected,
    held,
    front_ring,
    partial,
    up_out,
    up_in,
    down_out,
    down_in,
    across,
    routed,
    gathered,
    total,
    product_out,
    product_in,
    front_sem,
    local_sem,
    samples_send,
    samples_recv,
    product_send,
    product_recv,
    up_send,
    up_recv,
    down_send,
    down_recv,
    across_send,
    across_recv,
    routed_send,
    routed_recv,
    above_send,
    above_recv,
    below_send,
    below_recv,
):
    col = lax.axis_index("col")
    row = lax.axis_index("row")
    group = lax.axis_index("group")
    passes, local, half, depth = samples.shape
    block, tile = partial.shape[3:]
    height = fronts.shape[1]
    tiles = height // tile
    steps = passes * tiles
    last = cols - 1
    other_row = 1 - row

    barrier = pltpu.get_barrier_semaphore()

    def greet(device):
        pl.semaphore_signal(
            barrier, inc=1, device_id=device, device_id_type=pl.DeviceIdType.MESH
        )

    greet({"row": other_row})
    for shift in range(1, groups):
        greet({"group": lax.rem(group + shift, groups)})

    @pl.when(col > 0)
    def _():
        greet({"col": col - 1})

    @pl.when(col < last)
    def _():
        greet({"col": col + 1})

    def fetch(step):
        slot = lax.rem(step, FRONT_SLOTS)
        start = pl.multiple_of(lax.rem(step, tiles) * tile, tile)
        return pltpu.make_async_copy(
            fronts.at[:, pl.ds(start, tile), :], front_ring.at[slot], front_sem.at[slot]
        )

    for step in range(min(FRONT_SLOTS, steps)):
        fetch(step).start()

    pl.semaphore_wait(barrier, groups + jnp.minimum(col, 1) + jnp.minimum(last - col, 1))

    def own_half(turn):
        return held.at[turn, :, pl.ds(pl.multiple_of(row * half, half), half), :]

    def samples_copy(turn):
        return remote(
            samples.at[turn],
            own_half(turn),
            samples_send.at[turn],
            samples_recv.at[turn],
            {"row": other_row},
        )

    def samples_here(turn):
        return pltpu.make_async_copy(samples.at[turn], own_half(turn), local_sem.at[turn])

    for turn in range(passes):
        samples_copy(turn).start()
        samples_here(turn).start()

    total[...] = jnp.zeros_like(total)

    def live(step):
        return (step >= 0) & (step < steps)

    def spent(step):
        return (step >= DRAIN) & (step < steps + DRAIN)

    def up_copy(step, chunk):
        slot = lax.rem(step, SLOTS)
        return remote(
            up_out.at[slot, chunk],
            up_in.at[slot, chunk],
            up_send.at[slot, chunk],
            up_recv.at[slot, chunk],
            {"col": jnp.minimum(col + 1, last)},
        )

    def down_copy(step, chunk):
        slot = lax.rem(step, SLOTS)
        return remote(
            down_out.at[slot, chunk],
            down_in.at[slot, chunk],
            down_send.at[slot, chunk],
            down_recv.at[slot, chunk],
            {"col": jnp.maximum(col - 1, 0)},
        )

    def across_copy(step):
        slot = lax.rem(step, SLOTS)
        return remote(
            across.at[slot, row],
            across.at[slot, row],
            across_send.at[slot],
            across_recv.at[slot],
            {"row": other_row},
        )

    def routed_copy(step, shift):
        slot = lax.rem(step, SLOTS)
        return remote(
            routed.at[slot, group],
            routed.at[slot, group],
            routed_send.at[slot, shift],
            routed_recv.at[slot, shift],
            {"group": lax.rem(group + shift, groups)},
        )

    def above_copy(step, chunk):
        slot = lax.rem(step, GATHER_SLOTS)
        return remote(
            gathered.at[slot, :, chunk],
            gathered.at[slot, :, chunk],
            above_send.at[slot, chunk],
            above_recv.at[slot, chunk],
            {"col": jnp.minimum(col + 1, last)},
        )

    def below_copy(step, chunk):
        slot = lax.rem(step, GATHER_SLOTS)
        return remote(
            gathered.at[slot, :, chunk],
            gathered.at[slot, :, chunk],
            below_send.at[slot, chunk],
            below_recv.at[slot, chunk],
            {"col": jnp.maximum(col - 1, 0)},
        )

    def first_product(step):
        @pl.when(live(step))
        def _():
            turn = step // tiles

            @pl.when(lax.rem(step, tiles) == 0)
            def _():
                samples_here(turn).wait()
                samples_copy(turn).wait_recv()

            fetch(step).wait()
            slot = lax.rem(step, FRONT_SLOTS)
            into = lax.rem(step, PARTIAL_SLOTS)
            for front in range(local):
                value = lax.dot_general(
                    held[turn, front],
                    front_ring[slot, front],
                    (((1,), (1,)), ((), ())),
                    preferred_element_type=jnp.float32,
                )
                for chunk in range(cols):
                    partial[into, chunk, front] = value[chunk * block : (chunk + 1) * block]

    def hop(step, toward, edge, copy, out, received):
        @pl.when(spent(step))
        def _():
            for chunk in range(cols):

                @pl.when(toward(chunk))
                def _():
                    copy(step - DRAIN, chunk).wait_send()

        @pl.when(live(step))
        def _():
            slot = lax.rem(step, SLOTS)
            own = lax.rem(step, PARTIAL_SLOTS)
            for chunk in range(cols):

                @pl.when(toward(chunk))
                def _():
                    @pl.when(col == edge)
                    def _():
                        out[slot, chunk] = partial[own, chunk].astype(out.dtype)

                    @pl.when(col != edge)
                    def _():
                        copy(step, chunk).wait_recv()
                        out[slot, chunk] = (
                            partial[own, chunk] + received[slot, chunk].astype(jnp.float32)
                        ).astype(out.dtype)

                    copy(step, chunk).start()

    def finish(step):
        @pl.when(spent(step))
        def _():
            across_copy(step - DRAIN).wait_send()

        @pl.when(live(step))
        def _():
            slot = lax.rem(step, SLOTS)
            own = lax.rem(step, PARTIAL_SLOTS)
            turn = step // tiles
            lanes = pl.ds(pl.multiple_of(lax.rem(step, tiles) * tile, tile), tile)

            def store(value):
                for front in range(local):
                    out = (value[front] * keep[front : front + 1, lanes]).astype(sampled.dtype)
                    sampled[front, turn, :, lanes] = out
                    across[slot, row, front] = out

            @pl.when(col == 0)
            def _():
                down_copy(step, col).wait_recv()
                store(partial[own, col] + down_in[slot, col].astype(jnp.float32))

            @pl.when(col == last)
            def _():
                up_copy(step, col).wait_recv()
                store(partial[own, col] + up_in[slot, col].astype(jnp.float32))

            @pl.when((col > 0) & (col < last))
            def _():
                up_copy(step, col).wait_recv()
                down_copy(step, col).wait_recv()
                store(
                    partial[own, col]
                    + up_in[slot, col].astype(jnp.float32)
                    + down_in[slot, col].astype(jnp.float32)
                )

            across_copy(step).start()

    def route(step):
        @pl.when(spent(step))
        def _():
            for shift in range(1, groups):
                routed_copy(step - DRAIN, shift).wait_send()

        @pl.when(live(step))
        def _():
            slot = lax.rem(step, SLOTS)
            across_copy(step).wait_recv()
            for front in range(local):
                value = from_blocks[front, 0] * across[slot, 0, front].astype(jnp.float32)
                value += from_blocks[front, 1] * across[slot, 1, front].astype(jnp.float32)
                routed[slot, group, front] = value.astype(routed.dtype)
            for shift in range(1, groups):
                routed_copy(step, shift).start()

    def send_chunk(step, chunk):
        @pl.when(col < last)
        def _():
            above_copy(step, chunk).start()

        @pl.when(col > 0)
        def _():
            below_copy(step, chunk).start()

    def drain_chunk(step, chunk):
        @pl.when(col < last)
        def _():
            above_copy(step, chunk).wait_send()

        @pl.when(col > 0)
        def _():
            below_copy(step, chunk).wait_send()

    def combine(step):
        @pl.when(spent(step))
        def _():
            drain_chunk(step - DRAIN, col)

        @pl.when(live(step))
        def _():
            slot = lax.rem(step, SLOTS)
            turn = step // tiles
            lanes = pl.ds(pl.multiple_of(lax.rem(step, tiles) * tile, tile), tile)
            for shift in range(1, groups):
                routed_copy(step, shift).wait_recv()
            parts = [
                routed[slot, source, front].astype(jnp.float32)
                for source in range(groups)
                for front in range(local)
            ]
            for parent in range(local):
                value = second[parent, turn, :, lanes].astype(jnp.float32)
                for number, part in enumerate(parts):
                    value += to_parents[parent, number] * part
                value = value * keep[parent : parent + 1, lanes]
                gathered[lax.rem(step, GATHER_SLOTS), parent, col] = value.astype(gathered.dtype)
            send_chunk(step, col)

    def forward(step, far):
        @pl.when((col >= far) & (col < last))
        def _():
            @pl.when(spent(step))
            def _():
                above_copy(step - DRAIN, col - far).wait_send()

        @pl.when((col + far <= last) & (col > 0))
        def _():
            @pl.when(spent(step))
            def _():
                below_copy(step - DRAIN, col + far).wait_send()

        @pl.when(live(step))
        def _():
            @pl.when(col >= far)
            def _():
                above_copy(step, col - far).wait_recv()

                @pl.when(col < last)
                def _():
                    above_copy(step, col - far).start()

            @pl.when(col + far <= last)
            def _():
                below_copy(step, col + far).wait_recv()

                @pl.when(col > 0)
                def _():
                    below_copy(step, col + far).start()

    def product_copy(turn):
        return remote(
            product_out.at[turn],
            product_in.at[turn],
            product_send.at[turn],
            product_recv.at[turn],
            {"row": other_row},
        )

    def second_product(step):
        @pl.when(live(step))
        def _():
            @pl.when(col == last)
            def _():
                above_copy(step, col - last).wait_recv()

            @pl.when(col == 0)
            def _():
                below_copy(step, col + last).wait_recv()

            turn = step // tiles
            slot = lax.rem(step, FRONT_SLOTS)
            from_slot = lax.rem(step, GATHER_SLOTS)
            width = depth // 6 if depth % 768 == 0 else depth
            for front in range(local):
                rows = gathered[from_slot, front].reshape(cols * block, tile)
                for begin in range(0, depth, width):
                    total[turn, front, :, begin : begin + width] += jnp.dot(
                        rows,
                        front_ring[slot, front, :, begin : begin + width],
                        preferred_element_type=jnp.float32,
                    )

            @pl.when(lax.rem(step, tiles) == tiles - 1)
            def _():
                theirs = pl.ds(pl.multiple_of(other_row * half, half), half)
                for front in range(local):
                    product_out[turn, front] = total[turn, front, theirs].astype(
                        product_out.dtype
                    )
                product_copy(turn).start()

            @pl.when(step + FRONT_SLOTS < steps)
            def _():
                fetch(step + FRONT_SLOTS).start()

    @pl.loop(0, steps + SECOND_LAG)
    def _(time):
        first_product(time)
        hop(time - col, lambda chunk: chunk > col, 0, up_copy, up_out, up_in)
        hop(time - (last - col), lambda chunk: chunk < col, last, down_copy, down_out, down_in)
        finish(time - last)
        second_product(time - SECOND_LAG)
        route(time - last - 1)
        combine(time - last - 2)
        for far in range(1, last):
            forward(time - last - 2 - far, far)

    for turn in range(passes):
        product_copy(turn).wait_recv()
        ours = pl.ds(pl.multiple_of(row * half, half), half)
        for front in range(local):
            projected[turn, front] = (
                total[turn, front, ours] + product_in[turn, front].astype(jnp.float32)
            ).astype(projected.dtype)
        product_copy(turn).wait_send()
        samples_copy(turn).wait_send()


def pipeline(fronts, samples, second_samples, front_sizes, parent_ids, block_maps):
    local, height, depth = fronts.shape
    groups, cols = lax.axis_size("group"), lax.axis_size("col")
    group, row, col = lax.axis_index("group"), lax.axis_index("row"), lax.axis_index("col")
    number, block_count = block_maps.shape
    own_sizes = lax.dynamic_slice_in_dim(front_sizes, group * local, local, 0)
    row_keep = row * height + jnp.arange(height, dtype=jnp.int32)[None, :] < own_sizes[:, None]
    col_keep = col * depth + jnp.arange(depth, dtype=jnp.int32)[None, :] < own_sizes[:, None]
    own_fronts = group * local + jnp.arange(local, dtype=jnp.int32)

    block = second_samples.shape[0] // PASSES
    half = samples.shape[0] // PASSES
    first = samples * col_keep[None].astype(samples.dtype)
    first = first.reshape(half // block, PASSES, block, local, depth)
    first = first.transpose(1, 3, 0, 2, 4).reshape(PASSES, local, half, depth)
    second = second_samples.reshape(PASSES, block, local, height).transpose(2, 0, 1, 3)
    own_maps = lax.dynamic_slice_in_dim(block_maps, group * local, local, 0)
    from_blocks = (own_maps == row).astype(jnp.float32)
    to_parents = (own_fronts[:, None] == parent_ids[None, :]).astype(jnp.float32)

    def vmem(*shape, dtype=jnp.bfloat16):
        return pltpu.VMEM(shape, dtype)

    def sems(*shape):
        return pltpu.SemaphoreType.DMA(shape)

    in_vmem = pl.BlockSpec(memory_space=pltpu.VMEM)
    in_smem = pl.BlockSpec(memory_space=pltpu.SMEM)
    anywhere = pl.BlockSpec(memory_space=pl.ANY)
    f32 = jnp.float32
    sampled, projected = pl.pallas_call(
        functools.partial(fused, cols, groups),
        out_shape=(
            jax.ShapeDtypeStruct((local, PASSES, block, height), jnp.bfloat16),
            jax.ShapeDtypeStruct((PASSES, local, half, depth), jnp.bfloat16),
        ),
        in_specs=[anywhere, anywhere, in_vmem, in_vmem, in_smem, in_smem],
        out_specs=(in_vmem, in_vmem),
        scratch_shapes=[
            vmem(PASSES, local, 2 * half, depth),
            vmem(FRONT_SLOTS, local, TILE, depth),
            vmem(PARTIAL_SLOTS, cols, local, block, TILE, dtype=f32),
            vmem(SLOTS, cols, local, block, TILE),
            vmem(SLOTS, cols, local, block, TILE),
            vmem(SLOTS, cols, local, block, TILE),
            vmem(SLOTS, cols, local, block, TILE),
            vmem(SLOTS, 2, local, block, TILE),
            vmem(SLOTS, groups, local, block, TILE),
            vmem(GATHER_SLOTS, local, cols, block, TILE),
            vmem(PASSES, local, 2 * half, depth, dtype=f32),
            vmem(PASSES, local, half, depth),
            vmem(PASSES, local, half, depth),
            sems(FRONT_SLOTS),
            sems(PASSES),
            sems(PASSES),
            sems(PASSES),
            sems(PASSES),
            sems(PASSES),
            sems(SLOTS, cols),
            sems(SLOTS, cols),
            sems(SLOTS, cols),
            sems(SLOTS, cols),
            sems(SLOTS),
            sems(SLOTS),
            sems(SLOTS, groups),
            sems(SLOTS, groups),
            sems(GATHER_SLOTS, cols),
            sems(GATHER_SLOTS, cols),
            sems(GATHER_SLOTS, cols),
            sems(GATHER_SLOTS, cols),
        ],
        compiler_params=pltpu.CompilerParams(
            collective_id=0, has_side_effects=True, vmem_limit_bytes=67043328
        ),
    )(first, fronts, second, row_keep.astype(f32), from_blocks, to_parents)
    sampled = sampled.transpose(1, 2, 0, 3).reshape(second_samples.shape)
    projected = projected.reshape(PASSES, local, half // block, block, depth)
    projected = projected.transpose(2, 0, 3, 1, 4).reshape(samples.shape)
    projected = projected * col_keep[None].astype(projected.dtype)
    return sampled, projected


def fits(mesh, fronts, samples, second_samples, block_maps):
    rows, cols = mesh.shape["row"], mesh.shape["col"]
    height, depth = fronts.shape[1] // rows, fronts.shape[2] // cols
    block = second_samples.shape[0] // cols // PASSES
    return (
        rows == 2
        and cols == 4
        and block_maps.shape[1] == rows
        and height % TILE == 0
        and depth % 128 == 0
        and second_samples.shape[0] % (cols * PASSES) == 0
        and block % 16 == 0
    )


def solution(mesh):
    placed = (
        P("group", "row", "col"),
        P("row", "group", "col"),
        P("col", "group", "row"),
        P(),
        P(),
        P(),
    )

    def step(fronts, samples, second_samples, front_sizes, parent_ids, block_maps):
        fast = fits(mesh, fronts, samples, second_samples, block_maps)
        return jax.shard_map(
            pipeline if fast else shards,
            mesh=mesh,
            in_specs=placed,
            out_specs=(P("col", "group", "row"), P("row", "group", "col")),
            check_vma=False,
        )(fronts, samples, second_samples, front_sizes, parent_ids, block_maps)

    return step
```

```python
import functools

import jax
import jax.numpy as jnp
from jax import lax
from jax.experimental import pallas as pl
from jax.experimental.pallas import tpu as pltpu
from jax.sharding import PartitionSpec as P

PASSES = 2
TILE = 256
BLOCK_TILES = 6
HOP = 2
ROUTE_LAG = 3 * HOP + 1
COMBINE_LAG = ROUTE_LAG + 2
SECOND_LAG = COMBINE_LAG + 3 * HOP
SLOTS = 8
OUT_SLOTS = 4
IN_SLOTS = 10
GATHER_SLOTS = 12
PARTIAL_SLOTS = 3 * HOP + 1
DRAIN = 2
FRONT_SLOTS = 12


def swap_pairs(count):
    return [(0, 1), (1, 0)] if count == 2 else None


def gather_row(value, count, own_row, axis):
    if count != 2:
        return lax.all_gather(value, "row", axis=axis, tiled=True)
    other = lax.ppermute(value, "row", swap_pairs(count))
    first = own_row == 0
    return jnp.concatenate(
        [jnp.where(first, value, other), jnp.where(first, other, value)], axis=axis
    )


def scatter_row(value, count, own_row):
    if count != 2:
        return lax.psum_scatter(
            value.astype(jnp.bfloat16), "row", scatter_dimension=0, tiled=True
        ).astype(jnp.float32)
    half = value.shape[0] // 2
    kept = lax.dynamic_slice_in_dim(value, own_row * half, half, 0)
    sent = lax.dynamic_slice_in_dim(value, (1 - own_row) * half, half, 0).astype(jnp.bfloat16)
    return kept + lax.ppermute(sent, "row", swap_pairs(count)).astype(jnp.float32)


def shards(fronts, samples, second_samples, front_sizes, parent_ids, block_maps):
    local_count, tile_rows, tile_cols = fronts.shape
    row_count = lax.axis_size("row")
    own_group = lax.axis_index("group")
    own_row = lax.axis_index("row")
    own_col = lax.axis_index("col")
    total_fronts = parent_ids.shape[0]
    block_count = block_maps.shape[1]
    own_sizes = lax.dynamic_slice_in_dim(front_sizes, own_group * local_count, local_count, 0)
    row_keep = (own_row * tile_rows + jnp.arange(tile_rows, dtype=jnp.int32))[None, :] < own_sizes[
        :, None
    ]
    col_keep = (own_col * tile_cols + jnp.arange(tile_cols, dtype=jnp.int32))[None, :] < own_sizes[
        :, None
    ]
    own_fronts = own_group * local_count + jnp.arange(local_count, dtype=jnp.int32)
    masked = gather_row(samples, row_count, own_row, 0) * col_keep[None].astype(jnp.bfloat16)
    partial_value = jnp.einsum("sfk,fmk->sfm", masked, fronts, preferred_element_type=jnp.float32)
    partial_value = (partial_value * row_keep[None].astype(jnp.float32)).astype(jnp.bfloat16)
    sampled = lax.psum_scatter(partial_value, "col", scatter_dimension=0, tiled=True)
    portion = lax.all_gather(sampled, ("group", "row"), axis=1, tiled=True)
    number = portion.shape[1]
    source = jnp.arange(number, dtype=jnp.int32)
    front_index = source // (local_count * row_count) * local_count + source % local_count
    block_index = source // local_count % row_count
    front_hot = (front_index[:, None] == jnp.arange(total_fronts, dtype=jnp.int32)[None, :]).astype(
        jnp.int32
    )
    parent = jnp.sum(front_hot * parent_ids[None, :], axis=1)
    map_rows = jnp.sum(front_hot[:, :, None] * block_maps[None, :, :], axis=1)
    block_hot = (jnp.arange(block_count, dtype=jnp.int32)[None, :] == block_index[:, None]).astype(
        jnp.int32
    )
    target = jnp.sum(block_hot * map_rows, axis=1)
    weight = (parent[:, None] == own_fronts[None, :]) & (target[:, None] == own_row)
    extension = jnp.einsum(
        "sik,ij->sjk", portion, weight.astype(jnp.bfloat16), preferred_element_type=jnp.float32
    )
    combined = (second_samples.astype(jnp.float32) + extension).astype(jnp.bfloat16)
    combined = combined * row_keep[None].astype(jnp.bfloat16)
    gathered = lax.all_gather(combined, "col", axis=0, tiled=True)
    product = jnp.einsum("sfm,fmk->sfk", gathered, fronts, preferred_element_type=jnp.float32)
    projected = scatter_row(product, row_count, own_row)
    projected = (projected * col_keep[None].astype(jnp.float32)).astype(jnp.bfloat16)
    return (sampled, projected)


def remote(source, target, send_sem, recv_sem, device):
    return pltpu.make_async_remote_copy(
        src_ref=source,
        dst_ref=target,
        send_sem=send_sem,
        recv_sem=recv_sem,
        device_id=device,
        device_id_type=pl.DeviceIdType.MESH,
    )


def fused(
    cols,
    groups,
    samples,
    fronts,
    second_from,
    sizes,
    parents,
    maps,
    sampled_to,
    projected_to,
    second,
    sampled,
    projected,
    held,
    front_ring,
    partial,
    up_out,
    up_in,
    down_out,
    down_in,
    across,
    routed,
    gathered,
    total,
    product_out,
    product_in,
    front_sem,
    local_sem,
    second_sem,
    sampled_sem,
    projected_sem,
    samples_send,
    samples_recv,
    product_send,
    product_recv,
    up_send,
    up_recv,
    down_send,
    down_recv,
    across_send,
    across_recv,
    routed_send,
    routed_recv,
    above_send,
    above_recv,
    below_send,
    below_recv,
):
    col = lax.axis_index("col")
    row = lax.axis_index("row")
    group = lax.axis_index("group")
    passes, local, half, depth = samples.shape
    block, tile = partial.shape[3:]
    height = fronts.shape[1]
    tiles = height // tile
    steps = passes * tiles
    last = cols - 1
    run = BLOCK_TILES
    other_row = 1 - row

    barrier = pltpu.get_barrier_semaphore()

    def greet(device):
        pl.semaphore_signal(
            barrier, inc=1, device_id=device, device_id_type=pl.DeviceIdType.MESH
        )

    greet({"row": other_row})
    for shift in range(1, groups):
        greet({"group": lax.rem(group + shift, groups)})

    @pl.when(col > 0)
    def _():
        greet({"col": col - 1})

    @pl.when(col < last)
    def _():
        greet({"col": col + 1})

    def place(step):
        begin = lax.div(step, passes * run)
        rest = lax.rem(step, passes * run)
        return lax.div(rest, run), begin * run + lax.rem(rest, run)

    def lanes_of(spot):
        return pl.ds(pl.multiple_of(spot * tile, tile), tile)

    def fetch(spot):
        slot = lax.rem(spot, FRONT_SLOTS)
        start = pl.multiple_of(spot * tile, tile)
        return pltpu.make_async_copy(
            fronts.at[:, pl.ds(start, tile), :], front_ring.at[slot], front_sem.at[slot]
        )

    own_fronts = [group * local + front for front in range(local)]
    own_sizes = [sizes[front] for front in own_fronts]
    number = parents.shape[0]

    def weight(condition):
        return jnp.where(condition, 1.0, 0.0).astype(jnp.float32)

    def kept(front, start, shape):
        at = start + lax.broadcasted_iota(jnp.int32, shape, len(shape) - 1)
        return at < own_sizes[front]

    second_copy = pltpu.make_async_copy(second_from, second, second_sem)
    sampled_copy = pltpu.make_async_copy(sampled, sampled_to, sampled_sem)

    pl.semaphore_wait(barrier, groups + jnp.minimum(col, 1) + jnp.minimum(last - col, 1))

    def own_half(turn):
        return held.at[turn, :, pl.ds(pl.multiple_of(row * half, half), half), :]

    def samples_copy(turn):
        return remote(
            samples.at[turn],
            own_half(turn),
            samples_send.at[turn],
            samples_recv.at[turn],
            {"row": other_row},
        )

    def samples_here(turn):
        return pltpu.make_async_copy(samples.at[turn], own_half(turn), local_sem.at[turn])

    for turn in range(passes):
        samples_copy(turn).start()
        samples_here(turn).start()
    for spot in range(min(FRONT_SLOTS, tiles)):
        fetch(spot).start()
    second_copy.start()
    total[...] = jnp.zeros_like(total)

    def live(step):
        return (step >= 0) & (step < steps)

    def spent(step):
        return (step >= DRAIN) & (step < steps + DRAIN)

    def up_copy(step, chunk):
        slot, into = lax.rem(step, OUT_SLOTS), lax.rem(step, IN_SLOTS)
        return remote(
            up_out.at[slot, chunk],
            up_in.at[into, chunk],
            up_send.at[slot, chunk],
            up_recv.at[into, chunk],
            {"col": jnp.minimum(col + 1, last)},
        )

    def down_copy(step, chunk):
        slot, into = lax.rem(step, OUT_SLOTS), lax.rem(step, IN_SLOTS)
        return remote(
            down_out.at[slot, chunk],
            down_in.at[into, chunk],
            down_send.at[slot, chunk],
            down_recv.at[into, chunk],
            {"col": jnp.maximum(col - 1, 0)},
        )

    def across_copy(step):
        slot = lax.rem(step, SLOTS)
        return remote(
            across.at[slot, row],
            across.at[slot, row],
            across_send.at[slot],
            across_recv.at[slot],
            {"row": other_row},
        )

    def routed_copy(step, shift):
        slot = lax.rem(step, SLOTS)
        return remote(
            routed.at[slot, group],
            routed.at[slot, group],
            routed_send.at[slot, shift],
            routed_recv.at[slot, shift],
            {"group": lax.rem(group + shift, groups)},
        )

    def above_copy(step, chunk):
        slot = lax.rem(step, GATHER_SLOTS)
        return remote(
            gathered.at[slot, :, chunk],
            gathered.at[slot, :, chunk],
            above_send.at[slot, chunk],
            above_recv.at[slot, chunk],
            {"col": jnp.minimum(col + 1, last)},
        )

    def below_copy(step, chunk):
        slot = lax.rem(step, GATHER_SLOTS)
        return remote(
            gathered.at[slot, :, chunk],
            gathered.at[slot, :, chunk],
            below_send.at[slot, chunk],
            below_recv.at[slot, chunk],
            {"col": jnp.maximum(col - 1, 0)},
        )

    def first_product(step):
        @pl.when(live(step))
        def _():
            turn, spot = place(step)

            @pl.when(spot == 0)
            def _():
                samples_here(turn).wait()
                samples_copy(turn).wait_recv()
                for front in range(local):
                    value = held[turn, front]
                    kept_here = kept(front, col * depth, value.shape)
                    held[turn, front] = jnp.where(kept_here, value, jnp.zeros_like(value))

            @pl.when(turn == 0)
            def _():
                fetch(spot).wait()

            slot = lax.rem(spot, FRONT_SLOTS)
            into = lax.rem(step, PARTIAL_SLOTS)
            for front in range(local):
                value = lax.dot_general(
                    held[turn, front],
                    front_ring[slot, front],
                    (((1,), (1,)), ((), ())),
                    preferred_element_type=jnp.float32,
                )
                for chunk in range(cols):
                    partial[into, chunk, front] = value[chunk * block : (chunk + 1) * block]

    def hop(step, order, toward, edge, copy, out, received):
        @pl.when(spent(step))
        def _():
            for chunk in range(cols):

                @pl.when(toward(chunk))
                def _():
                    copy(step - DRAIN, chunk).wait_send()

        @pl.when(live(step))
        def _():
            slot, into = lax.rem(step, OUT_SLOTS), lax.rem(step, IN_SLOTS)
            own = lax.rem(step, PARTIAL_SLOTS)
            for chunk in order:

                @pl.when(toward(chunk))
                def _():
                    @pl.when(col == edge)
                    def _():
                        out[slot, chunk] = partial[own, chunk].astype(out.dtype)

                    @pl.when(col != edge)
                    def _():
                        copy(step, chunk).wait_recv()
                        out[slot, chunk] = (
                            partial[own, chunk] + received[into, chunk].astype(jnp.float32)
                        ).astype(out.dtype)

                    copy(step, chunk).start()

    def finish(step):
        @pl.when(spent(step))
        def _():
            across_copy(step - DRAIN).wait_send()

        @pl.when(live(step))
        def _():
            slot, into = lax.rem(step, SLOTS), lax.rem(step, IN_SLOTS)
            own = lax.rem(step, PARTIAL_SLOTS)
            turn, spot = place(step)
            lanes = lanes_of(spot)

            def store(value):
                for front in range(local):
                    kept_here = kept(front, row * height + spot * tile, (block, tile))
                    out = jnp.where(kept_here, value[front], 0.0).astype(sampled.dtype)
                    sampled[front, turn, :, lanes] = out
                    across[slot, row, front] = out

            @pl.when(col == 0)
            def _():
                down_copy(step, col).wait_recv()
                store(partial[own, col] + down_in[into, col].astype(jnp.float32))

            @pl.when(col == last)
            def _():
                up_copy(step, col).wait_recv()
                store(partial[own, col] + up_in[into, col].astype(jnp.float32))

            @pl.when((col > 0) & (col < last))
            def _():
                up_copy(step, col).wait_recv()
                down_copy(step, col).wait_recv()
                store(
                    partial[own, col]
                    + up_in[into, col].astype(jnp.float32)
                    + down_in[into, col].astype(jnp.float32)
                )

            across_copy(step).start()

            @pl.when(step == steps - 1)
            def _():
                sampled_copy.start()

    def route(step):
        @pl.when(spent(step))
        def _():
            for shift in range(1, groups):
                routed_copy(step - DRAIN, shift).wait_send()

        @pl.when(live(step))
        def _():
            slot = lax.rem(step, SLOTS)
            across_copy(step).wait_recv()
            for front in range(local):
                at = own_fronts[front]
                value = weight(maps[0, at] == row) * across[slot, 0, front].astype(jnp.float32)
                value += weight(maps[1, at] == row) * across[slot, 1, front].astype(jnp.float32)
                routed[slot, group, front] = value.astype(routed.dtype)
            for shift in range(1, groups):
                routed_copy(step, shift).start()

    def send_chunk(step, chunk):
        @pl.when(col < last)
        def _():
            above_copy(step, chunk).start()

        @pl.when(col > 0)
        def _():
            below_copy(step, chunk).start()

    def drain_chunk(step, chunk):
        @pl.when(col < last)
        def _():
            above_copy(step, chunk).wait_send()

        @pl.when(col > 0)
        def _():
            below_copy(step, chunk).wait_send()

    def combine(step):
        @pl.when(spent(step))
        def _():
            drain_chunk(step - DRAIN, col)

        @pl.when(live(step))
        def _():
            slot = lax.rem(step, SLOTS)
            turn, spot = place(step)
            lanes = lanes_of(spot)
            @pl.when(step == 0)
            def _():
                second_copy.wait()

            for shift in range(1, groups):
                routed_copy(step, shift).wait_recv()
            parts = [
                routed[slot, source, front].astype(jnp.float32)
                for source in range(groups)
                for front in range(local)
            ]
            for parent in range(local):
                value = second[parent, turn, :, lanes].astype(jnp.float32)
                for child in range(number):
                    value += weight(parents[child] == own_fronts[parent]) * parts[child]
                value = jnp.where(
                    kept(parent, row * height + spot * tile, value.shape), value, 0.0
                )
                gathered[lax.rem(step, GATHER_SLOTS), parent, col] = value.astype(gathered.dtype)
            send_chunk(step, col)

    def forward(step, far):
        @pl.when((col >= far) & (col < last))
        def _():
            @pl.when(spent(step))
            def _():
                above_copy(step - DRAIN, col - far).wait_send()

        @pl.when((col + far <= last) & (col > 0))
        def _():
            @pl.when(spent(step))
            def _():
                below_copy(step - DRAIN, col + far).wait_send()

        @pl.when(live(step))
        def _():
            @pl.when((col >= far) & (col < last))
            def _():
                above_copy(step, col - far).wait_recv()
                above_copy(step, col - far).start()

            @pl.when((col + far <= last) & (col > 0))
            def _():
                below_copy(step, col + far).wait_recv()
                below_copy(step, col + far).start()

    def product_copy(turn):
        return remote(
            product_out.at[turn],
            product_in.at[turn],
            product_send.at[turn],
            product_recv.at[turn],
            {"row": other_row},
        )

    def second_product(step):
        @pl.when(live(step))
        def _():
            @pl.when(col == last)
            def _():
                for chunk in range(last):
                    above_copy(step, chunk).wait_recv()

            @pl.when(col == 0)
            def _():
                for chunk in range(1, cols):
                    below_copy(step, chunk).wait_recv()

            turn, spot = place(step)
            slot = lax.rem(spot, FRONT_SLOTS)
            from_slot = lax.rem(step, GATHER_SLOTS)
            width = depth // 6 if depth % 768 == 0 else depth
            for front in range(local):
                rows = gathered[from_slot, front].reshape(cols * block, tile)
                for begin in range(0, depth, width):
                    total[turn, front, :, begin : begin + width] += jnp.dot(
                        rows,
                        front_ring[slot, front, :, begin : begin + width],
                        preferred_element_type=jnp.float32,
                    )

            @pl.when(spot == tiles - 1)
            def _():
                theirs = pl.ds(pl.multiple_of(other_row * half, half), half)
                for front in range(local):
                    product_out[turn, front] = total[turn, front, theirs].astype(
                        product_out.dtype
                    )
                product_copy(turn).start()

            @pl.when((turn == passes - 1) & (spot + FRONT_SLOTS < tiles))
            def _():
                fetch(spot + FRONT_SLOTS).start()

    @pl.loop(0, steps + SECOND_LAG)
    def _(time):
        first_product(time)
        hop(time - HOP * col, range(cols - 1, -1, -1), lambda chunk: chunk > col, 0, up_copy, up_out, up_in)
        hop(time - HOP * (last - col), range(cols), lambda chunk: chunk < col, last, down_copy, down_out, down_in)
        finish(time - HOP * last)
        second_product(time - SECOND_LAG)
        route(time - ROUTE_LAG)
        combine(time - COMBINE_LAG)
        for far in range(1, last):
            forward(time - COMBINE_LAG - HOP * far, far)

    def projected_copy(turn):
        return pltpu.make_async_copy(
            projected.at[turn], projected_to.at[turn], projected_sem.at[turn]
        )

    for turn in range(passes):
        product_copy(turn).wait_recv()
        ours = pl.ds(pl.multiple_of(row * half, half), half)
        for front in range(local):
            value = total[turn, front, ours] + product_in[turn, front].astype(jnp.float32)
            kept_here = kept(front, col * depth, value.shape)
            projected[turn, front] = jnp.where(kept_here, value, 0.0).astype(projected.dtype)
        projected_copy(turn).start()
    for turn in range(passes):
        product_copy(turn).wait_send()
        samples_copy(turn).wait_send()
        projected_copy(turn).wait()
    sampled_copy.wait()


def pipeline(fronts, samples, second_samples, front_sizes, parent_ids, block_maps):
    local, height, depth = fronts.shape
    groups, cols = lax.axis_size("group"), lax.axis_size("col")
    block = second_samples.shape[0] // PASSES
    half = samples.shape[0] // PASSES
    first = samples.reshape(half // block, PASSES, block, local, depth)
    first = first.transpose(1, 3, 0, 2, 4).reshape(PASSES, local, half, depth)
    second = second_samples.reshape(PASSES, block, local, height).transpose(2, 0, 1, 3)
    def vmem(*shape, dtype=jnp.bfloat16):
        return pltpu.VMEM(shape, dtype)

    def sems(*shape):
        return pltpu.SemaphoreType.DMA(shape)

    in_smem = pl.BlockSpec(memory_space=pltpu.SMEM)
    anywhere = pl.BlockSpec(memory_space=pl.ANY)
    f32 = jnp.float32
    sampled, projected = pl.pallas_call(
        functools.partial(fused, cols, groups),
        out_shape=(
            jax.ShapeDtypeStruct((local, PASSES, block, height), jnp.bfloat16),
            jax.ShapeDtypeStruct((PASSES, local, half, depth), jnp.bfloat16),
        ),
        in_specs=[anywhere, anywhere, anywhere, in_smem, in_smem, in_smem],
        out_specs=(anywhere, anywhere),
        scratch_shapes=[
            vmem(local, PASSES, block, height),
            vmem(local, PASSES, block, height),
            vmem(PASSES, local, half, depth),
            vmem(PASSES, local, 2 * half, depth),
            vmem(FRONT_SLOTS, local, TILE, depth),
            vmem(PARTIAL_SLOTS, cols, local, block, TILE, dtype=f32),
            vmem(OUT_SLOTS, cols, local, block, TILE),
            vmem(IN_SLOTS, cols, local, block, TILE),
            vmem(OUT_SLOTS, cols, local, block, TILE),
            vmem(IN_SLOTS, cols, local, block, TILE),
            vmem(SLOTS, 2, local, block, TILE),
            vmem(SLOTS, groups, local, block, TILE),
            vmem(GATHER_SLOTS, local, cols, block, TILE),
            vmem(PASSES, local, 2 * half, depth, dtype=f32),
            vmem(PASSES, local, half, depth),
            vmem(PASSES, local, half, depth),
            sems(FRONT_SLOTS),
            sems(PASSES),
            pltpu.SemaphoreType.DMA,
            pltpu.SemaphoreType.DMA,
            sems(PASSES),
            sems(PASSES),
            sems(PASSES),
            sems(PASSES),
            sems(PASSES),
            sems(OUT_SLOTS, cols),
            sems(IN_SLOTS, cols),
            sems(OUT_SLOTS, cols),
            sems(IN_SLOTS, cols),
            sems(SLOTS),
            sems(SLOTS),
            sems(SLOTS, groups),
            sems(SLOTS, groups),
            sems(GATHER_SLOTS, cols),
            sems(GATHER_SLOTS, cols),
            sems(GATHER_SLOTS, cols),
            sems(GATHER_SLOTS, cols),
        ],
        compiler_params=pltpu.CompilerParams(
            collective_id=0, has_side_effects=True, vmem_limit_bytes=67043328
        ),
    )(first, fronts, second, front_sizes, parent_ids, block_maps.T)
    sampled = sampled.transpose(1, 2, 0, 3).reshape(second_samples.shape)
    projected = projected.reshape(PASSES, local, half // block, block, depth)
    projected = projected.transpose(2, 0, 3, 1, 4).reshape(samples.shape)
    return sampled, projected


def fits(mesh, fronts, samples, second_samples, block_maps):
    rows, cols = mesh.shape["row"], mesh.shape["col"]
    height, depth = fronts.shape[1] // rows, fronts.shape[2] // cols
    block = second_samples.shape[0] // cols // PASSES
    return (
        rows == 2
        and cols == 4
        and block_maps.shape[1] == rows
        and height % TILE == 0
        and depth % 128 == 0
        and second_samples.shape[0] % (cols * PASSES) == 0
        and block % 16 == 0
    )


def solution(mesh):
    placed = (
        P("group", "row", "col"),
        P("row", "group", "col"),
        P("col", "group", "row"),
        P(),
        P(),
        P(),
    )

    def step(fronts, samples, second_samples, front_sizes, parent_ids, block_maps):
        fast = fits(mesh, fronts, samples, second_samples, block_maps)
        return jax.shard_map(
            pipeline if fast else shards,
            mesh=mesh,
            in_specs=placed,
            out_specs=(P("col", "group", "row"), P("row", "group", "col")),
            check_vma=False,
        )(fronts, samples, second_samples, front_sizes, parent_ids, block_maps)

    return step
```

```python
import functools

import jax
import jax.numpy as jnp
from jax import lax
from jax.experimental import pallas as pl
from jax.experimental.pallas import tpu as pltpu
from jax.sharding import PartitionSpec as P

QUARTERS = 4
TILE = 256
EDGE_TILES = 8
EARLY_QUARTERS = 2
FIRST_PIECE = 3
FINISH_LAG = 4
ROUTE_LAG = 6
COMBINE_LAG = 7
FORWARD_LAGS = (9, 10)
SECOND_LAG = 12
SLOTS = 8
OUT_SLOTS = 4
IN_SLOTS = 8
GATHER_SLOTS = 12
PARTIAL_SLOTS = 17
DRAIN = 2
FRONT_SLOTS = 13


def swap_pairs(count):
    return [(0, 1), (1, 0)] if count == 2 else None


def gather_row(value, count, own_row, axis):
    if count != 2:
        return lax.all_gather(value, "row", axis=axis, tiled=True)
    other = lax.ppermute(value, "row", swap_pairs(count))
    first = own_row == 0
    return jnp.concatenate(
        [jnp.where(first, value, other), jnp.where(first, other, value)], axis=axis
    )


def scatter_row(value, count, own_row):
    if count != 2:
        return lax.psum_scatter(
            value.astype(jnp.bfloat16), "row", scatter_dimension=0, tiled=True
        ).astype(jnp.float32)
    half = value.shape[0] // 2
    kept = lax.dynamic_slice_in_dim(value, own_row * half, half, 0)
    sent = lax.dynamic_slice_in_dim(value, (1 - own_row) * half, half, 0).astype(jnp.bfloat16)
    return kept + lax.ppermute(sent, "row", swap_pairs(count)).astype(jnp.float32)


def shards(fronts, samples, second_samples, front_sizes, parent_ids, block_maps):
    local_count, tile_rows, tile_cols = fronts.shape
    row_count = lax.axis_size("row")
    own_group = lax.axis_index("group")
    own_row = lax.axis_index("row")
    own_col = lax.axis_index("col")
    total_fronts = parent_ids.shape[0]
    block_count = block_maps.shape[1]
    own_sizes = lax.dynamic_slice_in_dim(front_sizes, own_group * local_count, local_count, 0)
    row_keep = (own_row * tile_rows + jnp.arange(tile_rows, dtype=jnp.int32))[None, :] < own_sizes[
        :, None
    ]
    col_keep = (own_col * tile_cols + jnp.arange(tile_cols, dtype=jnp.int32))[None, :] < own_sizes[
        :, None
    ]
    own_fronts = own_group * local_count + jnp.arange(local_count, dtype=jnp.int32)
    masked = gather_row(samples, row_count, own_row, 0) * col_keep[None].astype(jnp.bfloat16)
    partial_value = jnp.einsum("sfk,fmk->sfm", masked, fronts, preferred_element_type=jnp.float32)
    partial_value = (partial_value * row_keep[None].astype(jnp.float32)).astype(jnp.bfloat16)
    sampled = lax.psum_scatter(partial_value, "col", scatter_dimension=0, tiled=True)
    portion = lax.all_gather(sampled, ("group", "row"), axis=1, tiled=True)
    number = portion.shape[1]
    source = jnp.arange(number, dtype=jnp.int32)
    front_index = source // (local_count * row_count) * local_count + source % local_count
    block_index = source // local_count % row_count
    front_hot = (front_index[:, None] == jnp.arange(total_fronts, dtype=jnp.int32)[None, :]).astype(
        jnp.int32
    )
    parent = jnp.sum(front_hot * parent_ids[None, :], axis=1)
    map_rows = jnp.sum(front_hot[:, :, None] * block_maps[None, :, :], axis=1)
    block_hot = (jnp.arange(block_count, dtype=jnp.int32)[None, :] == block_index[:, None]).astype(
        jnp.int32
    )
    target = jnp.sum(block_hot * map_rows, axis=1)
    weight = (parent[:, None] == own_fronts[None, :]) & (target[:, None] == own_row)
    extension = jnp.einsum(
        "sik,ij->sjk", portion, weight.astype(jnp.bfloat16), preferred_element_type=jnp.float32
    )
    combined = (second_samples.astype(jnp.float32) + extension).astype(jnp.bfloat16)
    combined = combined * row_keep[None].astype(jnp.bfloat16)
    gathered = lax.all_gather(combined, "col", axis=0, tiled=True)
    product = jnp.einsum("sfm,fmk->sfk", gathered, fronts, preferred_element_type=jnp.float32)
    projected = scatter_row(product, row_count, own_row)
    projected = (projected * col_keep[None].astype(jnp.float32)).astype(jnp.bfloat16)
    return (sampled, projected)


def remote(source, target, send_sem, recv_sem, device):
    return pltpu.make_async_remote_copy(
        src_ref=source,
        dst_ref=target,
        send_sem=send_sem,
        recv_sem=recv_sem,
        device_id=device,
        device_id_type=pl.DeviceIdType.MESH,
    )


def fused(
    cols,
    groups,
    samples,
    fronts,
    second_from,
    sizes,
    parents,
    maps,
    sampled_to,
    projected_to,
    second,
    held,
    front_ring,
    partial,
    up_out,
    up_in,
    down_out,
    down_in,
    across,
    routed,
    gathered,
    total,
    product_in,
    front_sem,
    local_sem,
    second_sem,
    sampled_sem,
    projected_sem,
    samples_send,
    samples_recv,
    product_send,
    product_recv,
    up_send,
    up_recv,
    down_send,
    down_recv,
    across_send,
    across_recv,
    routed_send,
    routed_recv,
    above_send,
    above_recv,
    below_send,
    below_recv,
):
    col = lax.axis_index("col")
    row = lax.axis_index("row")
    group = lax.axis_index("group")
    quarters, local, half, depth = samples.shape
    block, tile = partial.shape[4:]
    pieces = half // block
    height = fronts.shape[1]
    tiles = height // tile
    steps = quarters * tiles // 2
    last = cols - 1
    edge_steps = quarters * EDGE_TILES // 2
    tail = steps - edge_steps
    other_row = 1 - row

    barrier = pltpu.get_barrier_semaphore()

    def greet(device):
        pl.semaphore_signal(
            barrier, inc=1, device_id=device, device_id_type=pl.DeviceIdType.MESH
        )

    greet({"row": other_row})
    for shift in range(1, groups):
        greet({"group": lax.rem(group + shift, groups)})

    @pl.when(col > 0)
    def _():
        greet({"col": col - 1})

    @pl.when(col < last)
    def _():
        greet({"col": col + 1})

    def narrow(step):
        return (step < edge_steps) | (step >= tail)

    def place(step, part):
        within = jnp.where(step < edge_steps, step, step - tail)
        first = jnp.where(step < edge_steps, 0, tiles - EDGE_TILES)
        pairs = EDGE_TILES // 2
        middle = jnp.maximum(step - edge_steps, 0)
        edge = narrow(step)
        within = jnp.where(edge, within, 0)
        quarter = jnp.where(
            edge, lax.div(within, pairs), 2 * lax.rem(middle, quarters // 2) + part
        )
        spot = jnp.where(
            edge,
            first + 2 * lax.rem(within, pairs) + part,
            EDGE_TILES + lax.div(middle, quarters // 2),
        )
        return quarter, spot

    def lanes_of(spot):
        return pl.ds(pl.multiple_of(spot * tile, tile), tile)

    def fetch(spot):
        slot = lax.rem(spot, FRONT_SLOTS)
        start = pl.multiple_of(spot * tile, tile)
        return pltpu.make_async_copy(
            fronts.at[:, pl.ds(start, tile), :], front_ring.at[slot], front_sem.at[slot]
        )

    own_fronts = [group * local + front for front in range(local)]
    own_sizes = [sizes[front] for front in own_fronts]
    number = parents.shape[0]

    def weight(condition):
        return jnp.where(condition, 1.0, 0.0).astype(jnp.float32)

    def kept(front, start, shape):
        at = start + lax.broadcasted_iota(jnp.int32, shape, len(shape) - 1)
        return at < own_sizes[front]

    second_copy = pltpu.make_async_copy(second_from, second, second_sem)

    pl.semaphore_wait(barrier, groups + jnp.minimum(col, 1) + jnp.minimum(last - col, 1))

    def samples_copy(quarter, front, piece):
        at = pl.multiple_of(row * half + piece * block, block)
        return remote(
            samples.at[quarter, front, pl.ds(piece * block, block), :],
            held.at[quarter, front, pl.ds(at, block), :],
            samples_send.at[quarter, front, piece],
            samples_recv.at[quarter, front, piece],
            {"row": other_row},
        )

    def samples_here(quarter):
        ours = pl.ds(pl.multiple_of(row * half, half), half)
        return pltpu.make_async_copy(
            samples.at[quarter], held.at[quarter, :, ours, :], local_sem.at[quarter]
        )

    every_piece = [(front, piece) for front in range(local) for piece in range(pieces)]
    for quarter in range(EARLY_QUARTERS):
        for front, piece in every_piece:
            samples_copy(quarter, front, piece).start()
    for quarter in range(quarters):
        samples_here(quarter).start()
    for spot in range(min(FRONT_SLOTS, tiles)):
        fetch(spot).start()
    second_copy.start()
    total[...] = jnp.zeros_like(total)

    def live(step):
        return (step >= 0) & (step < steps)

    def spent(step):
        return (step >= DRAIN) & (step < steps + DRAIN)

    def up_copy(step, chunk):
        slot, into = lax.rem(step, OUT_SLOTS), lax.rem(step, IN_SLOTS)
        return remote(
            up_out.at[slot, chunk],
            up_in.at[into, chunk],
            up_send.at[slot, chunk],
            up_recv.at[into, chunk],
            {"col": jnp.minimum(col + 1, last)},
        )

    def down_copy(step, chunk):
        slot, into = lax.rem(step, OUT_SLOTS), lax.rem(step, IN_SLOTS)
        return remote(
            down_out.at[slot, chunk],
            down_in.at[into, chunk],
            down_send.at[slot, chunk],
            down_recv.at[into, chunk],
            {"col": jnp.maximum(col - 1, 0)},
        )

    def across_copy(step):
        slot = lax.rem(step, SLOTS)
        return remote(
            across.at[slot, row],
            across.at[slot, row],
            across_send.at[slot],
            across_recv.at[slot],
            {"row": other_row},
        )

    def routed_copy(step, shift):
        slot = lax.rem(step, SLOTS)
        return remote(
            routed.at[slot, group],
            routed.at[slot, group],
            routed_send.at[slot, shift],
            routed_recv.at[slot, shift],
            {"group": lax.rem(group + shift, groups)},
        )

    def above_copy(step, chunk):
        slot = lax.rem(step, GATHER_SLOTS)
        return remote(
            gathered.at[slot, :, chunk],
            gathered.at[slot, :, chunk],
            above_send.at[slot, chunk],
            above_recv.at[slot, chunk],
            {"col": jnp.minimum(col + 1, last)},
        )

    def below_copy(step, chunk):
        slot = lax.rem(step, GATHER_SLOTS)
        return remote(
            gathered.at[slot, :, chunk],
            gathered.at[slot, :, chunk],
            below_send.at[slot, chunk],
            below_recv.at[slot, chunk],
            {"col": jnp.maximum(col - 1, 0)},
        )

    def first_product(step):
        @pl.when(live(step))
        def _():
            spots = [place(step, part) for part in range(2)]
            quarter, spot = spots[0]
            size = cols * block

            @pl.when((step < edge_steps) & (spot == 0))
            def _():
                samples_here(quarter).wait()
                for front, piece in every_piece:
                    samples_copy(quarter, front, piece).wait_recv()
                for front in range(local):
                    value = held[quarter, front]
                    kept_here = kept(front, col * depth, value.shape)
                    held[quarter, front] = jnp.where(kept_here, value, jnp.zeros_like(value))

            @pl.when(quarter == 0)
            def _():
                fetch(spot).wait()

            def product(rows, spot, front):
                return lax.dot_general(
                    rows,
                    front_ring[lax.rem(spot, FRONT_SLOTS), front],
                    (((1,), (1,)), ((), ())),
                    preferred_element_type=jnp.float32,
                )

            def keep(value, front, part, at):
                into = lax.rem(at, PARTIAL_SLOTS)
                for chunk in range(cols):
                    partial[into, chunk, front, part] = value[
                        chunk * block : (chunk + 1) * block
                    ].astype(partial.dtype)

            def whole(front, spot):
                rows = held[:, front].reshape(quarters * size, depth)
                value = product(rows, spot, front)
                return [value[quarter * size : (quarter + 1) * size] for quarter in range(quarters)]

            @pl.when(narrow(step) & (quarter == 0))
            def _():
                fetch(spots[1][1]).wait()

            @pl.when(step < edge_steps)
            def _():
                for front in range(local):
                    for part, (_, tile_spot) in enumerate(spots):
                        keep(product(held[quarter, front], tile_spot, front), front, part, step)

            @pl.when((step >= tail) & (quarter == 0))
            def _():
                for front in range(local):
                    for part, (_, tile_spot) in enumerate(spots):
                        for index, value in enumerate(whole(front, tile_spot)):
                            keep(value, front, part, step + index * (EDGE_TILES // 2))

            @pl.when((step >= edge_steps) & (step < tail) & (quarter == 0))
            def _():
                for front in range(local):
                    for index, value in enumerate(whole(front, spot)):
                        keep(value, front, index % 2, step + index // 2)

    def hop(step, order, toward, edge, copy, out, received):
        @pl.when(spent(step))
        def _():
            for chunk in range(cols):

                @pl.when(toward(chunk))
                def _():
                    copy(step - DRAIN, chunk).wait_send()

        @pl.when(live(step))
        def _():
            slot, into = lax.rem(step, OUT_SLOTS), lax.rem(step, IN_SLOTS)
            own = lax.rem(step, PARTIAL_SLOTS)
            for chunk in order:

                @pl.when(toward(chunk))
                def _():
                    @pl.when(col == edge)
                    def _():
                        out[slot, chunk] = partial[own, chunk].astype(out.dtype)

                    @pl.when(col != edge)
                    def _():
                        copy(step, chunk).wait_recv()
                        out[slot, chunk] = (
                            partial[own, chunk].astype(jnp.float32)
                            + received[into, chunk].astype(jnp.float32)
                        ).astype(out.dtype)

                    copy(step, chunk).start()

    def sampled_copies(step):
        slot = lax.rem(step, SLOTS)
        spots = [place(step, part) for part in range(2)]
        return [
            pltpu.make_async_copy(
                across.at[slot, row, :, part],
                sampled_to.at[:, quarter, :, lanes_of(spot)],
                sampled_sem.at[slot, part],
            )
            for part, (quarter, spot) in enumerate(spots)
        ]

    def finish(step):
        @pl.when(spent(step))
        def _():
            across_copy(step - DRAIN).wait_send()
            for copy in sampled_copies(step - DRAIN):
                copy.wait()

        @pl.when(live(step))
        def _():
            slot, into = lax.rem(step, SLOTS), lax.rem(step, IN_SLOTS)
            own = lax.rem(step, PARTIAL_SLOTS)
            spots = [place(step, part) for part in range(2)]

            def store(value):
                for front in range(local):
                    for part, (quarter, spot) in enumerate(spots):
                        kept_here = kept(front, row * height + spot * tile, (block, tile))
                        out = jnp.where(kept_here, value[front, part], 0.0).astype(across.dtype)
                        across[slot, row, front, part] = out

            @pl.when(col == 0)
            def _():
                down_copy(step, col).wait_recv()
                store(partial[own, col].astype(jnp.float32) + down_in[into, col].astype(jnp.float32))

            @pl.when(col == last)
            def _():
                up_copy(step, col).wait_recv()
                store(partial[own, col].astype(jnp.float32) + up_in[into, col].astype(jnp.float32))

            @pl.when((col > 0) & (col < last))
            def _():
                up_copy(step, col).wait_recv()
                down_copy(step, col).wait_recv()
                store(
                    partial[own, col].astype(jnp.float32)
                    + up_in[into, col].astype(jnp.float32)
                    + down_in[into, col].astype(jnp.float32)
                )

            across_copy(step).start()

            for copy in sampled_copies(step):
                copy.start()

    def route(step):
        @pl.when(spent(step))
        def _():
            for shift in range(1, groups):
                routed_copy(step - DRAIN, shift).wait_send()

        @pl.when(live(step))
        def _():
            slot = lax.rem(step, SLOTS)
            across_copy(step).wait_recv()
            for front in range(local):
                at = own_fronts[front]
                value = weight(maps[0, at] == row) * across[slot, 0, front].astype(jnp.float32)
                value += weight(maps[1, at] == row) * across[slot, 1, front].astype(jnp.float32)
                routed[slot, group, front] = value.astype(routed.dtype)
            for shift in range(1, groups):
                routed_copy(step, shift).start()

    def send_chunk(step, chunk):
        @pl.when(col < last)
        def _():
            above_copy(step, chunk).start()

        @pl.when(col > 0)
        def _():
            below_copy(step, chunk).start()

    def drain_chunk(step, chunk):
        @pl.when(col < last)
        def _():
            above_copy(step, chunk).wait_send()

        @pl.when(col > 0)
        def _():
            below_copy(step, chunk).wait_send()

    def combine(step):
        @pl.when(spent(step))
        def _():
            drain_chunk(step - DRAIN, col)

        @pl.when(live(step))
        def _():
            slot = lax.rem(step, SLOTS)
            spots = [place(step, part) for part in range(2)]

            @pl.when(step == 0)
            def _():
                second_copy.wait()

            for shift in range(1, groups):
                routed_copy(step, shift).wait_recv()
            parts = [
                routed[slot, source, front].astype(jnp.float32)
                for source in range(groups)
                for front in range(local)
            ]
            for parent in range(local):
                extension = weight(parents[0] == own_fronts[parent]) * parts[0]
                for child in range(1, number):
                    extension += weight(parents[child] == own_fronts[parent]) * parts[child]
                for part, (quarter, spot) in enumerate(spots):
                    value = second[parent, quarter, :, lanes_of(spot)].astype(jnp.float32)
                    value += extension[part]
                    kept_here = kept(parent, row * height + spot * tile, value.shape)
                    gathered[lax.rem(step, GATHER_SLOTS), parent, col, part] = jnp.where(
                        kept_here, value, 0.0
                    ).astype(gathered.dtype)
            send_chunk(step, col)

    def forward(step, far):
        @pl.when((col >= far) & (col < last))
        def _():
            @pl.when(spent(step))
            def _():
                above_copy(step - DRAIN, col - far).wait_send()

        @pl.when((col + far <= last) & (col > 0))
        def _():
            @pl.when(spent(step))
            def _():
                below_copy(step - DRAIN, col + far).wait_send()

        @pl.when(live(step))
        def _():
            @pl.when((col >= far) & (col < last))
            def _():
                above_copy(step, col - far).wait_recv()
                above_copy(step, col - far).start()

            @pl.when((col + far <= last) & (col > 0))
            def _():
                below_copy(step, col + far).wait_recv()
                below_copy(step, col + far).start()

    def product_copy(quarter, front, piece):
        rows = pl.ds(piece * block, block)
        return remote(
            held.at[quarter, front, rows, :],
            product_in.at[quarter, front, rows, :],
            product_send.at[quarter, front, piece],
            product_recv.at[quarter, front, piece],
            {"row": other_row},
        )

    def send_product(quarter, front, piece):
        theirs = pl.ds(pl.multiple_of(other_row * half + piece * block, block), block)
        held[quarter, front, pl.ds(piece * block, block), :] = total[
            quarter, front, theirs, :
        ].astype(held.dtype)
        product_copy(quarter, front, piece).start()

    def exchange(time):
        late = len(every_piece) * (quarters - EARLY_QUARTERS)

        @pl.when((time >= FIRST_PIECE) & (time < FIRST_PIECE + late))
        def _():
            number = time - FIRST_PIECE
            quarter = EARLY_QUARTERS + lax.div(number, len(every_piece))
            rest = lax.rem(number, len(every_piece))
            for index, (front, piece) in enumerate(every_piece):

                @pl.when(rest == index)
                def _():
                    samples_copy(quarter, front, piece).start()

        done = time - SECOND_LAG - tail + 1 - EDGE_TILES // 2

        @pl.when((done >= 0) & (done <= (quarters - 1) * len(every_piece)))
        def _():
            quarter = lax.div(done, len(every_piece))
            rest = lax.rem(done, len(every_piece))
            for index, (front, piece) in enumerate(every_piece):

                @pl.when((rest == index) | (quarter == quarters - 1))
                def _():
                    send_product(quarter, front, piece)

    def second_product(step):
        @pl.when(live(step))
        def _():
            @pl.when(col == last)
            def _():
                for chunk in range(last):
                    above_copy(step, chunk).wait_recv()

            @pl.when(col == 0)
            def _():
                for chunk in range(1, cols):
                    below_copy(step, chunk).wait_recv()

            spots = [place(step, part) for part in range(2)]
            quarter, spot = spots[0]
            from_slot = lax.rem(step, GATHER_SLOTS)
            size = cols * block
            width = depth // 6 if depth % 768 == 0 else depth

            def rows_of(front, part):
                return gathered[from_slot, front, :, part].reshape(size, tile)

            def product(rows, spot, front, begin):
                return jnp.dot(
                    rows,
                    front_ring[lax.rem(spot, FRONT_SLOTS), front, :, begin : begin + width],
                    preferred_element_type=jnp.float32,
                )

            @pl.when(narrow(step))
            def _():
                for front in range(local):
                    rows = [rows_of(front, part) for part in range(2)]
                    for begin in range(0, depth, width):
                        total[quarter, front, :, begin : begin + width] += product(
                            rows[0], spot, front, begin
                        ) + product(rows[1], spots[1][1], front, begin)

                @pl.when(quarter == quarters - 1)
                def _():
                    for _, done in spots:

                        @pl.when(done + FRONT_SLOTS < tiles)
                        def _():
                            fetch(done + FRONT_SLOTS).start()

            @pl.when(jnp.logical_not(narrow(step)))
            def _():
                for front in range(local):
                    rows = jnp.concatenate([rows_of(front, part) for part in range(2)], axis=0)
                    for begin in range(0, depth, width):
                        value = product(rows, spot, front, begin)
                        for part in range(2):
                            total[quarter + part, front, :, begin : begin + width] += value[
                                part * size : (part + 1) * size
                            ]

                @pl.when((quarter == quarters - 2) & (spot + FRONT_SLOTS < tiles))
                def _():
                    fetch(spot + FRONT_SLOTS).start()

    odd = lax.rem(col, 2)

    def up_hop(time):
        hop(
            time - lax.div(3 * col, 2),
            range(cols - 1, 0, -1),
            lambda chunk: chunk > col,
            0,
            up_copy,
            up_out,
            up_in,
        )

    def down_hop(time):
        hop(
            time - lax.div(3 * (last - col), 2),
            range(last),
            lambda chunk: chunk < col,
            last,
            down_copy,
            down_out,
            down_in,
        )

    @pl.loop(0, steps + SECOND_LAG)
    def _(time):
        first_product(time)
        pl.when(odd == 0)(lambda: up_hop(time))
        pl.when(odd == 1)(lambda: down_hop(time))
        route(time - ROUTE_LAG)
        forward(time - FORWARD_LAGS[0], 1)
        second_product(time - SECOND_LAG)
        pl.when(odd == 1)(lambda: up_hop(time))
        pl.when(odd == 0)(lambda: down_hop(time))
        finish(time - FINISH_LAG)
        combine(time - COMBINE_LAG)
        forward(time - FORWARD_LAGS[1], 2)
        exchange(time)

    def projected_copy(quarter):
        return pltpu.make_async_copy(
            product_in.at[quarter], projected_to.at[quarter], projected_sem.at[quarter]
        )

    for quarter in range(quarters):
        ours = pl.ds(pl.multiple_of(row * half, half), half)
        for front in range(local):
            for piece in range(pieces):
                product_copy(quarter, front, piece).wait_recv()
            value = total[quarter, front, ours] + product_in[quarter, front].astype(jnp.float32)
            kept_here = kept(front, col * depth, value.shape)
            product_in[quarter, front] = jnp.where(kept_here, value, 0.0).astype(
                product_in.dtype
            )
        projected_copy(quarter).start()
    for quarter in range(quarters):
        for front, piece in every_piece:
            product_copy(quarter, front, piece).wait_send()
            samples_copy(quarter, front, piece).wait_send()
        projected_copy(quarter).wait()


def pipeline(fronts, samples, second_samples, front_sizes, parent_ids, block_maps):
    local, height, depth = fronts.shape
    groups, cols = lax.axis_size("group"), lax.axis_size("col")
    block = second_samples.shape[0] // QUARTERS
    half = samples.shape[0] // QUARTERS
    first = samples.reshape(half // block, QUARTERS, block, local, depth)
    first = first.transpose(1, 3, 0, 2, 4).reshape(QUARTERS, local, half, depth)
    second = second_samples.reshape(QUARTERS, block, local, height).transpose(2, 0, 1, 3)
    def vmem(*shape, dtype=jnp.bfloat16):
        return pltpu.VMEM(shape, dtype)

    def sems(*shape):
        return pltpu.SemaphoreType.DMA(shape)

    in_smem = pl.BlockSpec(memory_space=pltpu.SMEM)
    anywhere = pl.BlockSpec(memory_space=pl.ANY)
    f32 = jnp.float32
    sampled, projected = pl.pallas_call(
        functools.partial(fused, cols, groups),
        out_shape=(
            jax.ShapeDtypeStruct((local, QUARTERS, block, height), jnp.bfloat16),
            jax.ShapeDtypeStruct((QUARTERS, local, half, depth), jnp.bfloat16),
        ),
        in_specs=[anywhere, anywhere, anywhere, in_smem, in_smem, in_smem],
        out_specs=(anywhere, anywhere),
        scratch_shapes=[
            vmem(local, QUARTERS, block, height),
            vmem(QUARTERS, local, 2 * half, depth),
            vmem(FRONT_SLOTS, local, TILE, depth),
            vmem(PARTIAL_SLOTS, cols, local, 2, block, TILE),
            vmem(OUT_SLOTS, cols, local, 2, block, TILE),
            vmem(IN_SLOTS, cols, local, 2, block, TILE),
            vmem(OUT_SLOTS, cols, local, 2, block, TILE),
            vmem(IN_SLOTS, cols, local, 2, block, TILE),
            vmem(SLOTS, 2, local, 2, block, TILE),
            vmem(SLOTS, groups, local, 2, block, TILE),
            vmem(GATHER_SLOTS, local, cols, 2, block, TILE),
            vmem(QUARTERS, local, 2 * half, depth, dtype=f32),
            vmem(QUARTERS, local, half, depth),
            sems(FRONT_SLOTS),
            sems(QUARTERS),
            pltpu.SemaphoreType.DMA,
            sems(SLOTS, 2),
            sems(QUARTERS),
            sems(QUARTERS, local, half // block),
            sems(QUARTERS, local, half // block),
            sems(QUARTERS, local, half // block),
            sems(QUARTERS, local, half // block),
            sems(OUT_SLOTS, cols),
            sems(IN_SLOTS, cols),
            sems(OUT_SLOTS, cols),
            sems(IN_SLOTS, cols),
            sems(SLOTS),
            sems(SLOTS),
            sems(SLOTS, groups),
            sems(SLOTS, groups),
            sems(GATHER_SLOTS, cols),
            sems(GATHER_SLOTS, cols),
            sems(GATHER_SLOTS, cols),
            sems(GATHER_SLOTS, cols),
        ],
        compiler_params=pltpu.CompilerParams(
            collective_id=0, has_side_effects=True, vmem_limit_bytes=67043328
        ),
    )(first, fronts, second, front_sizes, parent_ids, block_maps.T)
    sampled = sampled.transpose(1, 2, 0, 3).reshape(second_samples.shape)
    projected = projected.reshape(QUARTERS, local, half // block, block, depth)
    projected = projected.transpose(2, 0, 3, 1, 4).reshape(samples.shape)
    return sampled, projected


def fits(mesh, fronts, samples, second_samples, block_maps):
    rows, cols = mesh.shape["row"], mesh.shape["col"]
    height, depth = fronts.shape[1] // rows, fronts.shape[2] // cols
    block = second_samples.shape[0] // cols // QUARTERS
    return (
        rows == 2
        and cols == 4
        and block_maps.shape[1] == rows
        and height % TILE == 0
        and height // TILE >= 2 * EDGE_TILES
        and depth % 128 == 0
        and second_samples.shape[0] % (cols * QUARTERS) == 0
        and block % 16 == 0
    )


def solution(mesh):
    placed = (
        P("group", "row", "col"),
        P("row", "group", "col"),
        P("col", "group", "row"),
        P(),
        P(),
        P(),
    )

    def step(fronts, samples, second_samples, front_sizes, parent_ids, block_maps):
        fast = fits(mesh, fronts, samples, second_samples, block_maps)
        return jax.shard_map(
            pipeline if fast else shards,
            mesh=mesh,
            in_specs=placed,
            out_specs=(P("col", "group", "row"), P("row", "group", "col")),
            check_vma=False,
        )(fronts, samples, second_samples, front_sizes, parent_ids, block_maps)

    return step
```

```python
import functools

import jax
import jax.numpy as jnp
from jax import lax
from jax.experimental import pallas as pl
from jax.experimental.pallas import tpu as pltpu
from jax.sharding import PartitionSpec as P

QUARTERS = 4
TILE = 256
EDGE_TILES = 8
EARLY_QUARTERS = 2
FIRST_PIECE = 1
FINISH_LAG = 4
ROUTE_LAG = 6
COMBINE_LAG = 7
FORWARD_LAGS = (9, 10)
SECOND_LAG = 12
SLOTS = 8
OUT_SLOTS = 4
IN_SLOTS = 8
GATHER_SLOTS = 12
PARTIAL_SLOTS = 18
DRAIN = 3
FRONT_SLOTS = 13


def swap_pairs(count):
    return [(0, 1), (1, 0)] if count == 2 else None


def gather_row(value, count, own_row, axis):
    if count != 2:
        return lax.all_gather(value, "row", axis=axis, tiled=True)
    other = lax.ppermute(value, "row", swap_pairs(count))
    first = own_row == 0
    return jnp.concatenate(
        [jnp.where(first, value, other), jnp.where(first, other, value)], axis=axis
    )


def scatter_row(value, count, own_row):
    if count != 2:
        return lax.psum_scatter(
            value.astype(jnp.bfloat16), "row", scatter_dimension=0, tiled=True
        ).astype(jnp.float32)
    half = value.shape[0] // 2
    kept = lax.dynamic_slice_in_dim(value, own_row * half, half, 0)
    sent = lax.dynamic_slice_in_dim(value, (1 - own_row) * half, half, 0).astype(jnp.bfloat16)
    return kept + lax.ppermute(sent, "row", swap_pairs(count)).astype(jnp.float32)


def shards(fronts, samples, second_samples, front_sizes, parent_ids, block_maps):
    local_count, tile_rows, tile_cols = fronts.shape
    row_count = lax.axis_size("row")
    own_group = lax.axis_index("group")
    own_row = lax.axis_index("row")
    own_col = lax.axis_index("col")
    total_fronts = parent_ids.shape[0]
    block_count = block_maps.shape[1]
    own_sizes = lax.dynamic_slice_in_dim(front_sizes, own_group * local_count, local_count, 0)
    row_keep = (own_row * tile_rows + jnp.arange(tile_rows, dtype=jnp.int32))[None, :] < own_sizes[
        :, None
    ]
    col_keep = (own_col * tile_cols + jnp.arange(tile_cols, dtype=jnp.int32))[None, :] < own_sizes[
        :, None
    ]
    own_fronts = own_group * local_count + jnp.arange(local_count, dtype=jnp.int32)
    masked = gather_row(samples, row_count, own_row, 0) * col_keep[None].astype(jnp.bfloat16)
    partial_value = jnp.einsum("sfk,fmk->sfm", masked, fronts, preferred_element_type=jnp.float32)
    partial_value = (partial_value * row_keep[None].astype(jnp.float32)).astype(jnp.bfloat16)
    sampled = lax.psum_scatter(partial_value, "col", scatter_dimension=0, tiled=True)
    portion = lax.all_gather(sampled, ("group", "row"), axis=1, tiled=True)
    number = portion.shape[1]
    source = jnp.arange(number, dtype=jnp.int32)
    front_index = source // (local_count * row_count) * local_count + source % local_count
    block_index = source // local_count % row_count
    front_hot = (front_index[:, None] == jnp.arange(total_fronts, dtype=jnp.int32)[None, :]).astype(
        jnp.int32
    )
    parent = jnp.sum(front_hot * parent_ids[None, :], axis=1)
    map_rows = jnp.sum(front_hot[:, :, None] * block_maps[None, :, :], axis=1)
    block_hot = (jnp.arange(block_count, dtype=jnp.int32)[None, :] == block_index[:, None]).astype(
        jnp.int32
    )
    target = jnp.sum(block_hot * map_rows, axis=1)
    weight = (parent[:, None] == own_fronts[None, :]) & (target[:, None] == own_row)
    extension = jnp.einsum(
        "sik,ij->sjk", portion, weight.astype(jnp.bfloat16), preferred_element_type=jnp.float32
    )
    combined = (second_samples.astype(jnp.float32) + extension).astype(jnp.bfloat16)
    combined = combined * row_keep[None].astype(jnp.bfloat16)
    gathered = lax.all_gather(combined, "col", axis=0, tiled=True)
    product = jnp.einsum("sfm,fmk->sfk", gathered, fronts, preferred_element_type=jnp.float32)
    projected = scatter_row(product, row_count, own_row)
    projected = (projected * col_keep[None].astype(jnp.float32)).astype(jnp.bfloat16)
    return (sampled, projected)


def remote(source, target, send_sem, recv_sem, device):
    return pltpu.make_async_remote_copy(
        src_ref=source,
        dst_ref=target,
        send_sem=send_sem,
        recv_sem=recv_sem,
        device_id=device,
        device_id_type=pl.DeviceIdType.MESH,
    )


def fused(
    cols,
    groups,
    samples,
    fronts,
    second_from,
    sizes,
    parents,
    maps,
    sampled_to,
    projected_to,
    second,
    held,
    front_ring,
    partial,
    up_out,
    up_in,
    down_out,
    down_in,
    across,
    routed,
    gathered,
    total,
    product_in,
    front_sem,
    local_sem,
    second_sem,
    sampled_sem,
    projected_sem,
    samples_send,
    samples_recv,
    product_send,
    product_recv,
    up_send,
    up_recv,
    down_send,
    down_recv,
    across_send,
    across_recv,
    routed_send,
    routed_recv,
    above_send,
    above_recv,
    below_send,
    below_recv,
):
    col = lax.axis_index("col")
    row = lax.axis_index("row")
    group = lax.axis_index("group")
    quarters, local, half, depth = samples.shape
    block, tile = partial.shape[4:]
    pieces = half // block
    height = fronts.shape[1]
    tiles = height // tile
    steps = quarters * tiles // 2
    last = cols - 1
    edge_steps = quarters * EDGE_TILES // 2
    tail = steps - edge_steps
    other_row = 1 - row

    barrier = pltpu.get_barrier_semaphore()

    def greet(device):
        pl.semaphore_signal(
            barrier, inc=1, device_id=device, device_id_type=pl.DeviceIdType.MESH
        )

    greet({"row": other_row})
    for shift in range(1, groups):
        greet({"group": lax.rem(group + shift, groups)})

    @pl.when(col > 0)
    def _():
        greet({"col": col - 1})

    @pl.when(col < last)
    def _():
        greet({"col": col + 1})

    def narrow(step):
        return (step < edge_steps) | (step >= tail)

    def place(step, part):
        within = jnp.where(step < edge_steps, step, step - tail)
        first = jnp.where(step < edge_steps, 0, tiles - EDGE_TILES)
        pairs = EDGE_TILES // 2
        middle = jnp.maximum(step - edge_steps, 0)
        edge = narrow(step)
        within = jnp.where(edge, within, 0)
        quarter = jnp.where(
            edge, lax.div(within, pairs), 2 * lax.rem(middle, quarters // 2) + part
        )
        spot = jnp.where(
            edge,
            first + 2 * lax.rem(within, pairs) + part,
            EDGE_TILES + lax.div(middle, quarters // 2),
        )
        return quarter, spot

    def lanes_of(spot):
        return pl.ds(pl.multiple_of(spot * tile, tile), tile)

    def fetch(spot):
        slot = lax.rem(spot, FRONT_SLOTS)
        start = pl.multiple_of(spot * tile, tile)
        return pltpu.make_async_copy(
            fronts.at[:, pl.ds(start, tile), :], front_ring.at[slot], front_sem.at[slot]
        )

    own_fronts = [group * local + front for front in range(local)]
    own_sizes = [sizes[front] for front in own_fronts]
    number = parents.shape[0]

    def weight(condition):
        return jnp.where(condition, 1.0, 0.0).astype(jnp.float32)

    def kept(front, start, shape):
        at = start + lax.broadcasted_iota(jnp.int32, shape, len(shape) - 1)
        return at < own_sizes[front]

    second_copy = pltpu.make_async_copy(second_from, second, second_sem)

    pl.semaphore_wait(barrier, groups + jnp.minimum(col, 1) + jnp.minimum(last - col, 1))

    def samples_copy(quarter, front, piece):
        at = pl.multiple_of(row * half + piece * block, block)
        return remote(
            samples.at[quarter, front, pl.ds(piece * block, block), :],
            held.at[quarter, front, pl.ds(at, block), :],
            samples_send.at[quarter, front, piece],
            samples_recv.at[quarter, front, piece],
            {"row": other_row},
        )

    def samples_here(quarter):
        ours = pl.ds(pl.multiple_of(row * half, half), half)
        return pltpu.make_async_copy(
            samples.at[quarter], held.at[quarter, :, ours, :], local_sem.at[quarter]
        )

    every_piece = [(front, piece) for front in range(local) for piece in range(pieces)]
    for quarter in range(EARLY_QUARTERS):
        for front, piece in every_piece:
            samples_copy(quarter, front, piece).start()
    for quarter in range(quarters):
        samples_here(quarter).start()
    for spot in range(min(FRONT_SLOTS, tiles)):
        fetch(spot).start()
    second_copy.start()
    total[...] = jnp.zeros_like(total)

    def live(step):
        return (step >= 0) & (step < steps)

    def spent(step):
        return (step >= DRAIN) & (step < steps + DRAIN)

    def up_copy(step, chunk):
        slot, into = lax.rem(step, OUT_SLOTS), lax.rem(step, IN_SLOTS)
        return remote(
            up_out.at[slot, chunk],
            up_in.at[into, chunk],
            up_send.at[slot, chunk],
            up_recv.at[into, chunk],
            {"col": jnp.minimum(col + 1, last)},
        )

    def down_copy(step, chunk):
        slot, into = lax.rem(step, OUT_SLOTS), lax.rem(step, IN_SLOTS)
        return remote(
            down_out.at[slot, chunk],
            down_in.at[into, chunk],
            down_send.at[slot, chunk],
            down_recv.at[into, chunk],
            {"col": jnp.maximum(col - 1, 0)},
        )

    def across_copy(step):
        slot = lax.rem(step, SLOTS)
        return remote(
            across.at[slot, row],
            across.at[slot, row],
            across_send.at[slot],
            across_recv.at[slot],
            {"row": other_row},
        )

    def routed_copy(step, shift):
        slot = lax.rem(step, SLOTS)
        return remote(
            routed.at[slot, group],
            routed.at[slot, group],
            routed_send.at[slot, shift],
            routed_recv.at[slot, shift],
            {"group": lax.rem(group + shift, groups)},
        )

    def above_copy(step, chunk):
        slot = lax.rem(step, GATHER_SLOTS)
        return remote(
            gathered.at[slot, :, chunk],
            gathered.at[slot, :, chunk],
            above_send.at[slot, chunk],
            above_recv.at[slot, chunk],
            {"col": jnp.minimum(col + 1, last)},
        )

    def below_copy(step, chunk):
        slot = lax.rem(step, GATHER_SLOTS)
        return remote(
            gathered.at[slot, :, chunk],
            gathered.at[slot, :, chunk],
            below_send.at[slot, chunk],
            below_recv.at[slot, chunk],
            {"col": jnp.maximum(col - 1, 0)},
        )

    def first_product(step, front):
        @pl.when(live(step))
        def _():
            spots = [place(step, part) for part in range(2)]
            quarter, spot = spots[0]
            size = cols * block

            @pl.when((step < edge_steps) & (spot == 0))
            def _():
                if front == 0:
                    samples_here(quarter).wait()
                for piece in range(pieces):
                    samples_copy(quarter, front, piece).wait_recv()
                value = held[quarter, front]
                kept_here = kept(front, col * depth, value.shape)
                held[quarter, front] = jnp.where(kept_here, value, jnp.zeros_like(value))

            if front == 0:

                @pl.when(quarter == 0)
                def _():
                    fetch(spot).wait()

                @pl.when(narrow(step) & (quarter == 0))
                def _():
                    fetch(spots[1][1]).wait()

            def product(rows, spot):
                return lax.dot_general(
                    rows,
                    front_ring[lax.rem(spot, FRONT_SLOTS), front],
                    (((1,), (1,)), ((), ())),
                    preferred_element_type=jnp.float32,
                )

            def keep(value, part, at):
                into = lax.rem(at, PARTIAL_SLOTS)
                for chunk in range(cols):
                    partial[into, chunk, front, part] = value[
                        chunk * block : (chunk + 1) * block
                    ].astype(partial.dtype)

            def whole(spot):
                rows = held[:, front].reshape(quarters * size, depth)
                value = product(rows, spot)
                return [value[quarter * size : (quarter + 1) * size] for quarter in range(quarters)]

            @pl.when(step < edge_steps)
            def _():
                for part, (_, tile_spot) in enumerate(spots):
                    keep(product(held[quarter, front], tile_spot), part, step)

            @pl.when((step >= tail) & (quarter == 0))
            def _():
                for part, (_, tile_spot) in enumerate(spots):
                    for index, value in enumerate(whole(tile_spot)):
                        keep(value, part, step + index * (EDGE_TILES // 2))

            @pl.when((step >= edge_steps) & (step < tail) & (quarter == 0))
            def _():
                for index, value in enumerate(whole(spot)):
                    keep(value, index % 2, step + index // 2)

    def hop(step, order, toward, edge, copy, out, received):
        @pl.when(spent(step))
        def _():
            for chunk in range(cols):

                @pl.when(toward(chunk))
                def _():
                    copy(step - DRAIN, chunk).wait_send()

        @pl.when(live(step))
        def _():
            slot, into = lax.rem(step, OUT_SLOTS), lax.rem(step, IN_SLOTS)
            own = lax.rem(step, PARTIAL_SLOTS)
            for chunk in order:

                @pl.when(toward(chunk))
                def _():
                    @pl.when(col == edge)
                    def _():
                        out[slot, chunk] = partial[own, chunk].astype(out.dtype)

                    @pl.when(col != edge)
                    def _():
                        copy(step, chunk).wait_recv()
                        out[slot, chunk] = (
                            partial[own, chunk].astype(jnp.float32)
                            + received[into, chunk].astype(jnp.float32)
                        ).astype(out.dtype)

                    copy(step, chunk).start()

    def sampled_copies(step):
        slot = lax.rem(step, SLOTS)
        spots = [place(step, part) for part in range(2)]
        return [
            pltpu.make_async_copy(
                across.at[slot, row, :, part],
                sampled_to.at[:, quarter, :, lanes_of(spot)],
                sampled_sem.at[slot, part],
            )
            for part, (quarter, spot) in enumerate(spots)
        ]

    def finish(step):
        @pl.when(spent(step))
        def _():
            across_copy(step - DRAIN).wait_send()
            for copy in sampled_copies(step - DRAIN):
                copy.wait()

        @pl.when(live(step))
        def _():
            slot, into = lax.rem(step, SLOTS), lax.rem(step, IN_SLOTS)
            own = lax.rem(step, PARTIAL_SLOTS)
            spots = [place(step, part) for part in range(2)]

            def store(value):
                for front in range(local):
                    for part, (quarter, spot) in enumerate(spots):
                        kept_here = kept(front, row * height + spot * tile, (block, tile))
                        out = jnp.where(kept_here, value[front, part], 0.0).astype(across.dtype)
                        across[slot, row, front, part] = out

            @pl.when(col == 0)
            def _():
                down_copy(step, col).wait_recv()
                store(partial[own, col].astype(jnp.float32) + down_in[into, col].astype(jnp.float32))

            @pl.when(col == last)
            def _():
                up_copy(step, col).wait_recv()
                store(partial[own, col].astype(jnp.float32) + up_in[into, col].astype(jnp.float32))

            @pl.when((col > 0) & (col < last))
            def _():
                up_copy(step, col).wait_recv()
                down_copy(step, col).wait_recv()
                store(
                    partial[own, col].astype(jnp.float32)
                    + up_in[into, col].astype(jnp.float32)
                    + down_in[into, col].astype(jnp.float32)
                )

            across_copy(step).start()

            for copy in sampled_copies(step):
                copy.start()

    def route(step):
        @pl.when(spent(step))
        def _():
            for shift in range(1, groups):
                routed_copy(step - DRAIN, shift).wait_send()

        @pl.when(live(step))
        def _():
            slot = lax.rem(step, SLOTS)
            across_copy(step).wait_recv()
            for front in range(local):
                at = own_fronts[front]
                value = weight(maps[0, at] == row) * across[slot, 0, front].astype(jnp.float32)
                value += weight(maps[1, at] == row) * across[slot, 1, front].astype(jnp.float32)
                routed[slot, group, front] = value.astype(routed.dtype)
            for shift in range(1, groups):
                routed_copy(step, shift).start()

    def send_chunk(step, chunk):
        @pl.when(col < last)
        def _():
            above_copy(step, chunk).start()

        @pl.when(col > 0)
        def _():
            below_copy(step, chunk).start()

    def drain_chunk(step, chunk):
        @pl.when(col < last)
        def _():
            above_copy(step, chunk).wait_send()

        @pl.when(col > 0)
        def _():
            below_copy(step, chunk).wait_send()

    def combine(step):
        @pl.when(spent(step))
        def _():
            drain_chunk(step - DRAIN, col)

        @pl.when(live(step))
        def _():
            slot = lax.rem(step, SLOTS)
            spots = [place(step, part) for part in range(2)]

            @pl.when(step == 0)
            def _():
                second_copy.wait()

            for shift in range(1, groups):
                routed_copy(step, shift).wait_recv()
            parts = [
                routed[slot, source, front].astype(jnp.float32)
                for source in range(groups)
                for front in range(local)
            ]
            for parent in range(local):
                extension = weight(parents[0] == own_fronts[parent]) * parts[0]
                for child in range(1, number):
                    extension += weight(parents[child] == own_fronts[parent]) * parts[child]
                for part, (quarter, spot) in enumerate(spots):
                    value = second[parent, quarter, :, lanes_of(spot)].astype(jnp.float32)
                    value += extension[part]
                    kept_here = kept(parent, row * height + spot * tile, value.shape)
                    gathered[lax.rem(step, GATHER_SLOTS), parent, col, part] = jnp.where(
                        kept_here, value, 0.0
                    ).astype(gathered.dtype)
            send_chunk(step, col)

    def forward(step, far):
        @pl.when((col >= far) & (col < last))
        def _():
            @pl.when(spent(step))
            def _():
                above_copy(step - DRAIN, col - far).wait_send()

        @pl.when((col + far <= last) & (col > 0))
        def _():
            @pl.when(spent(step))
            def _():
                below_copy(step - DRAIN, col + far).wait_send()

        @pl.when(live(step))
        def _():
            @pl.when((col >= far) & (col < last))
            def _():
                above_copy(step, col - far).wait_recv()
                above_copy(step, col - far).start()

            @pl.when((col + far <= last) & (col > 0))
            def _():
                below_copy(step, col + far).wait_recv()
                below_copy(step, col + far).start()

    def product_copy(quarter, front, piece):
        rows = pl.ds(piece * block, block)
        return remote(
            held.at[quarter, front, rows, :],
            product_in.at[quarter, front, rows, :],
            product_send.at[quarter, front, piece],
            product_recv.at[quarter, front, piece],
            {"row": other_row},
        )

    def send_product(quarter, front, piece):
        theirs = pl.ds(pl.multiple_of(other_row * half + piece * block, block), block)
        held[quarter, front, pl.ds(piece * block, block), :] = total[
            quarter, front, theirs, :
        ].astype(held.dtype)
        product_copy(quarter, front, piece).start()

    def exchange(time):
        late = len(every_piece) * (quarters - EARLY_QUARTERS)

        @pl.when((time >= FIRST_PIECE) & (time < FIRST_PIECE + late))
        def _():
            number = time - FIRST_PIECE
            quarter = EARLY_QUARTERS + lax.div(number, len(every_piece))
            rest = lax.rem(number, len(every_piece))
            for index, (front, piece) in enumerate(every_piece):

                @pl.when(rest == index)
                def _():
                    samples_copy(quarter, front, piece).start()

        done = time - SECOND_LAG - tail + 1 - EDGE_TILES // 2

        @pl.when((done >= 0) & (done <= (quarters - 1) * len(every_piece)))
        def _():
            quarter = lax.div(done, len(every_piece))
            rest = lax.rem(done, len(every_piece))
            for index, (front, piece) in enumerate(every_piece):

                @pl.when((rest == index) | (quarter == quarters - 1))
                def _():
                    send_product(quarter, front, piece)

    def second_product(step, front):
        @pl.when(live(step))
        def _():
            if front == 0:

                @pl.when(col == last)
                def _():
                    for chunk in range(last):
                        above_copy(step, chunk).wait_recv()

                @pl.when(col == 0)
                def _():
                    for chunk in range(1, cols):
                        below_copy(step, chunk).wait_recv()

            spots = [place(step, part) for part in range(2)]
            quarter, spot = spots[0]
            from_slot = lax.rem(step, GATHER_SLOTS)
            size = cols * block
            width = depth // 6 if depth % 768 == 0 else depth

            def rows_of(part):
                return gathered[from_slot, front, :, part].reshape(size, tile)

            def product(rows, spot, begin):
                return jnp.dot(
                    rows,
                    front_ring[lax.rem(spot, FRONT_SLOTS), front, :, begin : begin + width],
                    preferred_element_type=jnp.float32,
                )

            @pl.when(narrow(step))
            def _():
                rows = [rows_of(part) for part in range(2)]
                for begin in range(0, depth, width):
                    total[quarter, front, :, begin : begin + width] += product(
                        rows[0], spot, begin
                    ) + product(rows[1], spots[1][1], begin)

                if front == local - 1:

                    @pl.when(quarter == quarters - 1)
                    def _():
                        for _, done in spots:

                            @pl.when(done + FRONT_SLOTS < tiles)
                            def _():
                                fetch(done + FRONT_SLOTS).start()

            @pl.when(jnp.logical_not(narrow(step)))
            def _():
                rows = jnp.concatenate([rows_of(part) for part in range(2)], axis=0)
                for begin in range(0, depth, width):
                    value = product(rows, spot, begin)
                    for part in range(2):
                        total[quarter + part, front, :, begin : begin + width] += value[
                            part * size : (part + 1) * size
                        ]

                if front == local - 1:

                    @pl.when((quarter == quarters - 2) & (spot + FRONT_SLOTS < tiles))
                    def _():
                        fetch(spot + FRONT_SLOTS).start()

    odd = lax.rem(col, 2)

    def up_hop(time):
        hop(
            time - lax.div(3 * col, 2),
            range(cols - 1, 0, -1),
            lambda chunk: chunk > col,
            0,
            up_copy,
            up_out,
            up_in,
        )

    def down_hop(time):
        hop(
            time - lax.div(3 * (last - col), 2),
            range(last),
            lambda chunk: chunk < col,
            last,
            down_copy,
            down_out,
            down_in,
        )

    first_product(jnp.int32(0), 0)

    @pl.loop(0, steps + max(SECOND_LAG, FORWARD_LAGS[1] + DRAIN))
    def _(time):
        for front in range(1, local):
            first_product(time, front)
        pl.when(odd == 0)(lambda: up_hop(time))
        pl.when(odd == 1)(lambda: down_hop(time))
        forward(time - FORWARD_LAGS[0], 1)
        route(time - ROUTE_LAG)
        second_product(time - SECOND_LAG, 0)
        first_product(time + 1, 0)
        combine(time - COMBINE_LAG)
        forward(time - FORWARD_LAGS[1], 2)
        pl.when(odd == 1)(lambda: up_hop(time))
        pl.when(odd == 0)(lambda: down_hop(time))
        finish(time - FINISH_LAG)
        for front in range(1, local):
            second_product(time - SECOND_LAG, front)
        exchange(time)

    def projected_copy(quarter):
        return pltpu.make_async_copy(
            product_in.at[quarter], projected_to.at[quarter], projected_sem.at[quarter]
        )

    for quarter in range(quarters):
        ours = pl.ds(pl.multiple_of(row * half, half), half)
        for front in range(local):
            for piece in range(pieces):
                product_copy(quarter, front, piece).wait_recv()
            value = total[quarter, front, ours] + product_in[quarter, front].astype(jnp.float32)
            kept_here = kept(front, col * depth, value.shape)
            product_in[quarter, front] = jnp.where(kept_here, value, 0.0).astype(
                product_in.dtype
            )
        projected_copy(quarter).start()
    for quarter in range(quarters):
        for front, piece in every_piece:
            product_copy(quarter, front, piece).wait_send()
            samples_copy(quarter, front, piece).wait_send()
        projected_copy(quarter).wait()


def pipeline(fronts, samples, second_samples, front_sizes, parent_ids, block_maps):
    local, height, depth = fronts.shape
    groups, cols = lax.axis_size("group"), lax.axis_size("col")
    block = second_samples.shape[0] // QUARTERS
    half = samples.shape[0] // QUARTERS
    first = samples.reshape(half // block, QUARTERS, block, local, depth)
    first = first.transpose(1, 3, 0, 2, 4).reshape(QUARTERS, local, half, depth)
    second = second_samples.reshape(QUARTERS, block, local, height).transpose(2, 0, 1, 3)
    def vmem(*shape, dtype=jnp.bfloat16):
        return pltpu.VMEM(shape, dtype)

    def sems(*shape):
        return pltpu.SemaphoreType.DMA(shape)

    in_smem = pl.BlockSpec(memory_space=pltpu.SMEM)
    anywhere = pl.BlockSpec(memory_space=pl.ANY)
    f32 = jnp.float32
    sampled, projected = pl.pallas_call(
        functools.partial(fused, cols, groups),
        out_shape=(
            jax.ShapeDtypeStruct((local, QUARTERS, block, height), jnp.bfloat16),
            jax.ShapeDtypeStruct((QUARTERS, local, half, depth), jnp.bfloat16),
        ),
        in_specs=[anywhere, anywhere, anywhere, in_smem, in_smem, in_smem],
        out_specs=(anywhere, anywhere),
        scratch_shapes=[
            vmem(local, QUARTERS, block, height),
            vmem(QUARTERS, local, 2 * half, depth),
            vmem(FRONT_SLOTS, local, TILE, depth),
            vmem(PARTIAL_SLOTS, cols, local, 2, block, TILE),
            vmem(OUT_SLOTS, cols, local, 2, block, TILE),
            vmem(IN_SLOTS, cols, local, 2, block, TILE),
            vmem(OUT_SLOTS, cols, local, 2, block, TILE),
            vmem(IN_SLOTS, cols, local, 2, block, TILE),
            vmem(SLOTS, 2, local, 2, block, TILE),
            vmem(SLOTS, groups, local, 2, block, TILE),
            vmem(GATHER_SLOTS, local, cols, 2, block, TILE),
            vmem(QUARTERS, local, 2 * half, depth, dtype=f32),
            vmem(QUARTERS, local, half, depth),
            sems(FRONT_SLOTS),
            sems(QUARTERS),
            pltpu.SemaphoreType.DMA,
            sems(SLOTS, 2),
            sems(QUARTERS),
            sems(QUARTERS, local, half // block),
            sems(QUARTERS, local, half // block),
            sems(QUARTERS, local, half // block),
            sems(QUARTERS, local, half // block),
            sems(OUT_SLOTS, cols),
            sems(IN_SLOTS, cols),
            sems(OUT_SLOTS, cols),
            sems(IN_SLOTS, cols),
            sems(SLOTS),
            sems(SLOTS),
            sems(SLOTS, groups),
            sems(SLOTS, groups),
            sems(GATHER_SLOTS, cols),
            sems(GATHER_SLOTS, cols),
            sems(GATHER_SLOTS, cols),
            sems(GATHER_SLOTS, cols),
        ],
        compiler_params=pltpu.CompilerParams(
            collective_id=0, has_side_effects=True, vmem_limit_bytes=67043328
        ),
    )(first, fronts, second, front_sizes, parent_ids, block_maps.T)
    sampled = sampled.transpose(1, 2, 0, 3).reshape(second_samples.shape)
    projected = projected.reshape(QUARTERS, local, half // block, block, depth)
    projected = projected.transpose(2, 0, 3, 1, 4).reshape(samples.shape)
    return sampled, projected


def fits(mesh, fronts, samples, second_samples, block_maps):
    rows, cols = mesh.shape["row"], mesh.shape["col"]
    height, depth = fronts.shape[1] // rows, fronts.shape[2] // cols
    block = second_samples.shape[0] // cols // QUARTERS
    return (
        rows == 2
        and cols == 4
        and block_maps.shape[1] == rows
        and height % TILE == 0
        and height // TILE >= 2 * EDGE_TILES
        and depth % 128 == 0
        and second_samples.shape[0] % (cols * QUARTERS) == 0
        and block % 16 == 0
    )


def solution(mesh):
    placed = (
        P("group", "row", "col"),
        P("row", "group", "col"),
        P("col", "group", "row"),
        P(),
        P(),
        P(),
    )

    def step(fronts, samples, second_samples, front_sizes, parent_ids, block_maps):
        fast = fits(mesh, fronts, samples, second_samples, block_maps)
        return jax.shard_map(
            pipeline if fast else shards,
            mesh=mesh,
            in_specs=placed,
            out_specs=(P("col", "group", "row"), P("row", "group", "col")),
            check_vma=False,
        )(fronts, samples, second_samples, front_sizes, parent_ids, block_maps)

    return step
```

```python
import functools

import jax
import jax.numpy as jnp
from jax import lax
from jax.experimental import pallas as pl
from jax.experimental.pallas import tpu as pltpu
from jax.sharding import PartitionSpec as P

QUARTERS = 4
TILE = 256
EDGE_TILES = 8
EARLY_QUARTERS = 2
FIRST_PIECE = 2
FINISH_LAG = 4
ROUTE_LAG = 6
COMBINE_LAG = 7
FORWARD_LAGS = (9, 10)
SECOND_LAG = 12
SLOTS = 8
OUT_SLOTS = 4
IN_SLOTS = 8
GATHER_SLOTS = 12
PARTIAL_SLOTS = 18
DRAIN = 3
FRONT_SLOTS = 13


def swap_pairs(count):
    return [(0, 1), (1, 0)] if count == 2 else None


def gather_row(value, count, own_row, axis):
    if count != 2:
        return lax.all_gather(value, "row", axis=axis, tiled=True)
    other = lax.ppermute(value, "row", swap_pairs(count))
    first = own_row == 0
    return jnp.concatenate(
        [jnp.where(first, value, other), jnp.where(first, other, value)], axis=axis
    )


def scatter_row(value, count, own_row):
    if count != 2:
        return lax.psum_scatter(
            value.astype(jnp.bfloat16), "row", scatter_dimension=0, tiled=True
        ).astype(jnp.float32)
    half = value.shape[0] // 2
    kept = lax.dynamic_slice_in_dim(value, own_row * half, half, 0)
    sent = lax.dynamic_slice_in_dim(value, (1 - own_row) * half, half, 0).astype(jnp.bfloat16)
    return kept + lax.ppermute(sent, "row", swap_pairs(count)).astype(jnp.float32)


def shards(fronts, samples, second_samples, front_sizes, parent_ids, block_maps):
    local_count, tile_rows, tile_cols = fronts.shape
    row_count = lax.axis_size("row")
    own_group = lax.axis_index("group")
    own_row = lax.axis_index("row")
    own_col = lax.axis_index("col")
    total_fronts = parent_ids.shape[0]
    block_count = block_maps.shape[1]
    own_sizes = lax.dynamic_slice_in_dim(front_sizes, own_group * local_count, local_count, 0)
    row_keep = (own_row * tile_rows + jnp.arange(tile_rows, dtype=jnp.int32))[None, :] < own_sizes[
        :, None
    ]
    col_keep = (own_col * tile_cols + jnp.arange(tile_cols, dtype=jnp.int32))[None, :] < own_sizes[
        :, None
    ]
    own_fronts = own_group * local_count + jnp.arange(local_count, dtype=jnp.int32)
    masked = gather_row(samples, row_count, own_row, 0) * col_keep[None].astype(jnp.bfloat16)
    partial_value = jnp.einsum("sfk,fmk->sfm", masked, fronts, preferred_element_type=jnp.float32)
    partial_value = (partial_value * row_keep[None].astype(jnp.float32)).astype(jnp.bfloat16)
    sampled = lax.psum_scatter(partial_value, "col", scatter_dimension=0, tiled=True)
    portion = lax.all_gather(sampled, ("group", "row"), axis=1, tiled=True)
    number = portion.shape[1]
    source = jnp.arange(number, dtype=jnp.int32)
    front_index = source // (local_count * row_count) * local_count + source % local_count
    block_index = source // local_count % row_count
    front_hot = (front_index[:, None] == jnp.arange(total_fronts, dtype=jnp.int32)[None, :]).astype(
        jnp.int32
    )
    parent = jnp.sum(front_hot * parent_ids[None, :], axis=1)
    map_rows = jnp.sum(front_hot[:, :, None] * block_maps[None, :, :], axis=1)
    block_hot = (jnp.arange(block_count, dtype=jnp.int32)[None, :] == block_index[:, None]).astype(
        jnp.int32
    )
    target = jnp.sum(block_hot * map_rows, axis=1)
    weight = (parent[:, None] == own_fronts[None, :]) & (target[:, None] == own_row)
    extension = jnp.einsum(
        "sik,ij->sjk", portion, weight.astype(jnp.bfloat16), preferred_element_type=jnp.float32
    )
    combined = (second_samples.astype(jnp.float32) + extension).astype(jnp.bfloat16)
    combined = combined * row_keep[None].astype(jnp.bfloat16)
    gathered = lax.all_gather(combined, "col", axis=0, tiled=True)
    product = jnp.einsum("sfm,fmk->sfk", gathered, fronts, preferred_element_type=jnp.float32)
    projected = scatter_row(product, row_count, own_row)
    projected = (projected * col_keep[None].astype(jnp.float32)).astype(jnp.bfloat16)
    return (sampled, projected)


def remote(source, target, send_sem, recv_sem, device):
    return pltpu.make_async_remote_copy(
        src_ref=source,
        dst_ref=target,
        send_sem=send_sem,
        recv_sem=recv_sem,
        device_id=device,
        device_id_type=pl.DeviceIdType.MESH,
    )


def fused(
    cols,
    groups,
    samples,
    fronts,
    second_from,
    sizes,
    parents,
    maps,
    sampled_to,
    projected_to,
    second,
    held,
    front_ring,
    partial,
    up_out,
    up_in,
    down_out,
    down_in,
    across,
    routed,
    gathered,
    total,
    product_in,
    front_sem,
    local_sem,
    second_sem,
    sampled_sem,
    projected_sem,
    samples_send,
    samples_recv,
    product_send,
    product_recv,
    up_send,
    up_recv,
    down_send,
    down_recv,
    across_send,
    across_recv,
    routed_send,
    routed_recv,
    above_send,
    above_recv,
    below_send,
    below_recv,
):
    col = lax.axis_index("col")
    row = lax.axis_index("row")
    group = lax.axis_index("group")
    quarters, local, half, depth = samples.shape
    block, tile = partial.shape[4:]
    pieces = half // block
    height = fronts.shape[1]
    tiles = height // tile
    steps = quarters * tiles // 2
    last = cols - 1
    edge_steps = quarters * EDGE_TILES // 2
    tail = steps - edge_steps
    other_row = 1 - row

    barrier = pltpu.get_barrier_semaphore()

    def greet(device):
        pl.semaphore_signal(
            barrier, inc=1, device_id=device, device_id_type=pl.DeviceIdType.MESH
        )

    greet({"row": other_row})
    for shift in range(1, groups):
        greet({"group": lax.rem(group + shift, groups)})

    @pl.when(col > 0)
    def _():
        greet({"col": col - 1})

    @pl.when(col < last)
    def _():
        greet({"col": col + 1})

    def narrow(step):
        return (step < edge_steps) | (step >= tail)

    def place(step, part):
        within = jnp.where(step < edge_steps, step, step - tail)
        first = jnp.where(step < edge_steps, 0, tiles - EDGE_TILES)
        pairs = EDGE_TILES // 2
        middle = jnp.maximum(step - edge_steps, 0)
        edge = narrow(step)
        within = jnp.where(edge, within, 0)
        quarter = jnp.where(
            edge, lax.div(within, pairs), 2 * lax.rem(middle, quarters // 2) + part
        )
        spot = jnp.where(
            edge,
            first + 2 * lax.rem(within, pairs) + part,
            EDGE_TILES + lax.div(middle, quarters // 2),
        )
        return quarter, spot

    def lanes_of(spot):
        return pl.ds(pl.multiple_of(spot * tile, tile), tile)

    def fetch(spot):
        slot = lax.rem(spot, FRONT_SLOTS)
        start = pl.multiple_of(spot * tile, tile)
        return pltpu.make_async_copy(
            fronts.at[:, pl.ds(start, tile), :], front_ring.at[slot], front_sem.at[slot]
        )

    own_fronts = [group * local + front for front in range(local)]
    own_sizes = [sizes[front] for front in own_fronts]
    number = parents.shape[0]

    def weight(condition):
        return jnp.where(condition, 1.0, 0.0).astype(jnp.float32)

    def kept(front, start, shape):
        at = start + lax.broadcasted_iota(jnp.int32, shape, len(shape) - 1)
        return at < own_sizes[front]

    second_copy = pltpu.make_async_copy(second_from, second, second_sem)

    pl.semaphore_wait(barrier, groups + jnp.minimum(col, 1) + jnp.minimum(last - col, 1))

    def samples_copy(quarter, front, piece):
        at = pl.multiple_of(row * half + piece * block, block)
        return remote(
            samples.at[quarter, front, pl.ds(piece * block, block), :],
            held.at[quarter, front, pl.ds(at, block), :],
            samples_send.at[quarter, front, piece],
            samples_recv.at[quarter, front, piece],
            {"row": other_row},
        )

    def samples_here(quarter):
        ours = pl.ds(pl.multiple_of(row * half, half), half)
        return pltpu.make_async_copy(
            samples.at[quarter], held.at[quarter, :, ours, :], local_sem.at[quarter]
        )

    every_piece = [(front, piece) for front in range(local) for piece in range(pieces)]
    for quarter in range(EARLY_QUARTERS):
        for front, piece in every_piece:
            samples_copy(quarter, front, piece).start()
    for quarter in range(quarters):
        samples_here(quarter).start()
    for spot in range(min(FRONT_SLOTS, tiles)):
        fetch(spot).start()
    second_copy.start()
    total[...] = jnp.zeros_like(total)

    def live(step):
        return (step >= 0) & (step < steps)

    def spent(step):
        return (step >= DRAIN) & (step < steps + DRAIN)

    def up_copy(step, chunk):
        slot, into = lax.rem(step, OUT_SLOTS), lax.rem(step, IN_SLOTS)
        return remote(
            up_out.at[slot, chunk],
            up_in.at[into, chunk],
            up_send.at[slot, chunk],
            up_recv.at[into, chunk],
            {"col": jnp.minimum(col + 1, last)},
        )

    def down_copy(step, chunk):
        slot, into = lax.rem(step, OUT_SLOTS), lax.rem(step, IN_SLOTS)
        return remote(
            down_out.at[slot, chunk],
            down_in.at[into, chunk],
            down_send.at[slot, chunk],
            down_recv.at[into, chunk],
            {"col": jnp.maximum(col - 1, 0)},
        )

    def across_copy(step):
        slot = lax.rem(step, SLOTS)
        return remote(
            across.at[slot, row],
            across.at[slot, row],
            across_send.at[slot],
            across_recv.at[slot],
            {"row": other_row},
        )

    def routed_copy(step, shift):
        slot = lax.rem(step, SLOTS)
        return remote(
            routed.at[slot, group],
            routed.at[slot, group],
            routed_send.at[slot, shift],
            routed_recv.at[slot, shift],
            {"group": lax.rem(group + shift, groups)},
        )

    def above_copy(step, chunk):
        slot = lax.rem(step, GATHER_SLOTS)
        return remote(
            gathered.at[slot, :, chunk],
            gathered.at[slot, :, chunk],
            above_send.at[slot, chunk],
            above_recv.at[slot, chunk],
            {"col": jnp.minimum(col + 1, last)},
        )

    def below_copy(step, chunk):
        slot = lax.rem(step, GATHER_SLOTS)
        return remote(
            gathered.at[slot, :, chunk],
            gathered.at[slot, :, chunk],
            below_send.at[slot, chunk],
            below_recv.at[slot, chunk],
            {"col": jnp.maximum(col - 1, 0)},
        )

    def first_product(step, front):
        @pl.when(live(step))
        def _():
            spots = [place(step, part) for part in range(2)]
            quarter, spot = spots[0]
            size = cols * block

            @pl.when((step < edge_steps) & (spot == 0))
            def _():
                if front == 0:
                    samples_here(quarter).wait()
                for piece in range(pieces):
                    samples_copy(quarter, front, piece).wait_recv()
                value = held[quarter, front]
                kept_here = kept(front, col * depth, value.shape)
                held[quarter, front] = jnp.where(kept_here, value, jnp.zeros_like(value))

            if front == 0:

                @pl.when(quarter == 0)
                def _():
                    fetch(spot).wait()

                @pl.when(narrow(step) & (quarter == 0))
                def _():
                    fetch(spots[1][1]).wait()

            def product(rows, spot):
                return lax.dot_general(
                    rows,
                    front_ring[lax.rem(spot, FRONT_SLOTS), front],
                    (((1,), (1,)), ((), ())),
                    preferred_element_type=jnp.float32,
                )

            def keep(value, part, at):
                into = lax.rem(at, PARTIAL_SLOTS)
                for chunk in range(cols):
                    partial[into, chunk, front, part] = value[
                        chunk * block : (chunk + 1) * block
                    ].astype(partial.dtype)

            def whole(spot):
                rows = held[:, front].reshape(quarters * size, depth)
                value = product(rows, spot)
                return [value[quarter * size : (quarter + 1) * size] for quarter in range(quarters)]

            @pl.when(step < edge_steps)
            def _():
                for part, (_, tile_spot) in enumerate(spots):
                    keep(product(held[quarter, front], tile_spot), part, step)

            @pl.when((step >= tail) & (quarter == 0))
            def _():
                for part, (_, tile_spot) in enumerate(spots):
                    for index, value in enumerate(whole(tile_spot)):
                        keep(value, part, step + index * (EDGE_TILES // 2))

            @pl.when((step >= edge_steps) & (step < tail) & (quarter == 0))
            def _():
                for index, value in enumerate(whole(spot)):
                    keep(value, index % 2, step + index // 2)

    def hop(step, order, toward, edge, copy, out, received):
        @pl.when(spent(step))
        def _():
            for chunk in range(cols):

                @pl.when(toward(chunk))
                def _():
                    copy(step - DRAIN, chunk).wait_send()

        @pl.when(live(step))
        def _():
            slot, into = lax.rem(step, OUT_SLOTS), lax.rem(step, IN_SLOTS)
            own = lax.rem(step, PARTIAL_SLOTS)
            for chunk in order:

                @pl.when(toward(chunk))
                def _():
                    @pl.when(col == edge)
                    def _():
                        out[slot, chunk] = partial[own, chunk].astype(out.dtype)

                    @pl.when(col != edge)
                    def _():
                        copy(step, chunk).wait_recv()
                        out[slot, chunk] = (
                            partial[own, chunk].astype(jnp.float32)
                            + received[into, chunk].astype(jnp.float32)
                        ).astype(out.dtype)

                    copy(step, chunk).start()

    def sampled_copies(step):
        slot = lax.rem(step, SLOTS)
        spots = [place(step, part) for part in range(2)]
        return [
            pltpu.make_async_copy(
                across.at[slot, row, :, part],
                sampled_to.at[:, quarter, :, lanes_of(spot)],
                sampled_sem.at[slot, part],
            )
            for part, (quarter, spot) in enumerate(spots)
        ]

    def finish(step):
        @pl.when(spent(step))
        def _():
            across_copy(step - DRAIN).wait_send()
            for copy in sampled_copies(step - DRAIN):
                copy.wait()

        @pl.when(live(step))
        def _():
            slot, into = lax.rem(step, SLOTS), lax.rem(step, IN_SLOTS)
            own = lax.rem(step, PARTIAL_SLOTS)
            spots = [place(step, part) for part in range(2)]

            def store(value):
                for front in range(local):
                    for part, (quarter, spot) in enumerate(spots):
                        kept_here = kept(front, row * height + spot * tile, (block, tile))
                        out = jnp.where(kept_here, value[front, part], 0.0).astype(across.dtype)
                        across[slot, row, front, part] = out

            @pl.when(col == 0)
            def _():
                down_copy(step, col).wait_recv()
                store(partial[own, col].astype(jnp.float32) + down_in[into, col].astype(jnp.float32))

            @pl.when(col == last)
            def _():
                up_copy(step, col).wait_recv()
                store(partial[own, col].astype(jnp.float32) + up_in[into, col].astype(jnp.float32))

            @pl.when((col > 0) & (col < last))
            def _():
                up_copy(step, col).wait_recv()
                down_copy(step, col).wait_recv()
                store(
                    partial[own, col].astype(jnp.float32)
                    + up_in[into, col].astype(jnp.float32)
                    + down_in[into, col].astype(jnp.float32)
                )

            across_copy(step).start()

            for copy in sampled_copies(step):
                copy.start()

    def route(step):
        @pl.when(spent(step))
        def _():
            for shift in range(1, groups):
                routed_copy(step - DRAIN, shift).wait_send()

        @pl.when(live(step))
        def _():
            slot = lax.rem(step, SLOTS)
            across_copy(step).wait_recv()
            for front in range(local):
                at = own_fronts[front]
                value = weight(maps[0, at] == row) * across[slot, 0, front].astype(jnp.float32)
                value += weight(maps[1, at] == row) * across[slot, 1, front].astype(jnp.float32)
                routed[slot, group, front] = value.astype(routed.dtype)
            for shift in range(1, groups):
                routed_copy(step, shift).start()

    def send_chunk(step, chunk):
        @pl.when(col < last)
        def _():
            above_copy(step, chunk).start()

        @pl.when(col > 0)
        def _():
            below_copy(step, chunk).start()

    def drain_chunk(step, chunk):
        @pl.when(col < last)
        def _():
            above_copy(step, chunk).wait_send()

        @pl.when(col > 0)
        def _():
            below_copy(step, chunk).wait_send()

    def combine(step):
        @pl.when(spent(step))
        def _():
            drain_chunk(step - DRAIN, col)

        @pl.when(live(step))
        def _():
            slot = lax.rem(step, SLOTS)
            spots = [place(step, part) for part in range(2)]

            @pl.when(step == 0)
            def _():
                second_copy.wait()

            for shift in range(1, groups):
                routed_copy(step, shift).wait_recv()
            parts = [
                routed[slot, source, front].astype(jnp.float32)
                for source in range(groups)
                for front in range(local)
            ]
            for parent in range(local):
                extension = weight(parents[0] == own_fronts[parent]) * parts[0]
                for child in range(1, number):
                    extension += weight(parents[child] == own_fronts[parent]) * parts[child]
                for part, (quarter, spot) in enumerate(spots):
                    value = second[parent, quarter, :, lanes_of(spot)].astype(jnp.float32)
                    value += extension[part]
                    kept_here = kept(parent, row * height + spot * tile, value.shape)
                    gathered[lax.rem(step, GATHER_SLOTS), parent, col, part] = jnp.where(
                        kept_here, value, 0.0
                    ).astype(gathered.dtype)
            send_chunk(step, col)

    def forward(step, far):
        @pl.when((col >= far) & (col < last))
        def _():
            @pl.when(spent(step))
            def _():
                above_copy(step - DRAIN, col - far).wait_send()

        @pl.when((col + far <= last) & (col > 0))
        def _():
            @pl.when(spent(step))
            def _():
                below_copy(step - DRAIN, col + far).wait_send()

        @pl.when(live(step))
        def _():
            @pl.when((col >= far) & (col < last))
            def _():
                above_copy(step, col - far).wait_recv()
                above_copy(step, col - far).start()

            @pl.when((col + far <= last) & (col > 0))
            def _():
                below_copy(step, col + far).wait_recv()
                below_copy(step, col + far).start()

    def product_copy(quarter, front, piece):
        rows = pl.ds(piece * block, block)
        return remote(
            held.at[quarter, front, rows, :],
            product_in.at[quarter, front, rows, :],
            product_send.at[quarter, front, piece],
            product_recv.at[quarter, front, piece],
            {"row": other_row},
        )

    def send_product(quarter, front, piece):
        theirs = pl.ds(pl.multiple_of(other_row * half + piece * block, block), block)
        held[quarter, front, pl.ds(piece * block, block), :] = total[
            quarter, front, theirs, :
        ].astype(held.dtype)
        product_copy(quarter, front, piece).start()

    def exchange(time):
        late = len(every_piece) * (quarters - EARLY_QUARTERS)

        @pl.when((time >= FIRST_PIECE) & (time < FIRST_PIECE + late))
        def _():
            number = time - FIRST_PIECE
            quarter = EARLY_QUARTERS + lax.div(number, len(every_piece))
            rest = lax.rem(number, len(every_piece))
            for index, (front, piece) in enumerate(every_piece):

                @pl.when(rest == index)
                def _():
                    samples_copy(quarter, front, piece).start()

        done = time - SECOND_LAG - tail + 1 - EDGE_TILES // 2

        @pl.when((done >= 0) & (done <= (quarters - 1) * len(every_piece)))
        def _():
            quarter = lax.div(done, len(every_piece))
            rest = lax.rem(done, len(every_piece))
            for index, (front, piece) in enumerate(every_piece):

                @pl.when((rest == index) | (quarter == quarters - 1))
                def _():
                    send_product(quarter, front, piece)

    def second_product(step, front):
        @pl.when(live(step))
        def _():
            if front == 0:

                @pl.when(col == last)
                def _():
                    for chunk in range(last):
                        above_copy(step, chunk).wait_recv()

                @pl.when(col == 0)
                def _():
                    for chunk in range(1, cols):
                        below_copy(step, chunk).wait_recv()

            spots = [place(step, part) for part in range(2)]
            quarter, spot = spots[0]
            from_slot = lax.rem(step, GATHER_SLOTS)
            size = cols * block
            width = depth // 6 if depth % 768 == 0 else depth

            def rows_of(part):
                return gathered[from_slot, front, :, part].reshape(size, tile)

            def product(rows, spot, begin):
                return jnp.dot(
                    rows,
                    front_ring[lax.rem(spot, FRONT_SLOTS), front, :, begin : begin + width],
                    preferred_element_type=jnp.float32,
                )

            @pl.when(narrow(step))
            def _():
                rows = [rows_of(part) for part in range(2)]
                for begin in range(0, depth, width):
                    total[quarter, front, :, begin : begin + width] += product(
                        rows[0], spot, begin
                    ) + product(rows[1], spots[1][1], begin)

                if front == local - 1:

                    @pl.when(quarter == quarters - 1)
                    def _():
                        for _, done in spots:

                            @pl.when(done + FRONT_SLOTS < tiles)
                            def _():
                                fetch(done + FRONT_SLOTS).start()

            @pl.when(jnp.logical_not(narrow(step)))
            def _():
                rows = jnp.concatenate([rows_of(part) for part in range(2)], axis=0)
                for begin in range(0, depth, width):
                    value = product(rows, spot, begin)
                    for part in range(2):
                        total[quarter + part, front, :, begin : begin + width] += value[
                            part * size : (part + 1) * size
                        ]

                if front == local - 1:

                    @pl.when((quarter == quarters - 2) & (spot + FRONT_SLOTS < tiles))
                    def _():
                        fetch(spot + FRONT_SLOTS).start()

    odd = lax.rem(col, 2)

    def up_hop(time):
        hop(
            time - lax.div(3 * col, 2),
            range(cols - 1, 0, -1),
            lambda chunk: chunk > col,
            0,
            up_copy,
            up_out,
            up_in,
        )

    def down_hop(time):
        hop(
            time - lax.div(3 * (last - col), 2),
            range(last),
            lambda chunk: chunk < col,
            last,
            down_copy,
            down_out,
            down_in,
        )

    first_product(jnp.int32(0), 0)

    @pl.loop(0, steps + max(SECOND_LAG, FORWARD_LAGS[1] + DRAIN))
    def _(time):
        for front in range(1, local):
            first_product(time, front)
        pl.when(odd == 0)(lambda: up_hop(time))
        pl.when(odd == 1)(lambda: down_hop(time))
        forward(time - FORWARD_LAGS[0], 1)
        route(time - ROUTE_LAG)
        second_product(time - SECOND_LAG, 0)
        first_product(time + 1, 0)
        combine(time - COMBINE_LAG)
        forward(time - FORWARD_LAGS[1], 2)
        pl.when(odd == 1)(lambda: up_hop(time))
        pl.when(odd == 0)(lambda: down_hop(time))
        finish(time - FINISH_LAG)
        for front in range(1, local):
            second_product(time - SECOND_LAG, front)
        exchange(time)

    def projected_copy(quarter):
        return pltpu.make_async_copy(
            product_in.at[quarter], projected_to.at[quarter], projected_sem.at[quarter]
        )

    for quarter in range(quarters):
        ours = pl.ds(pl.multiple_of(row * half, half), half)
        for front in range(local):
            for piece in range(pieces):
                product_copy(quarter, front, piece).wait_recv()
            value = total[quarter, front, ours] + product_in[quarter, front].astype(jnp.float32)
            kept_here = kept(front, col * depth, value.shape)
            product_in[quarter, front] = jnp.where(kept_here, value, 0.0).astype(
                product_in.dtype
            )
        projected_copy(quarter).start()
    for quarter in range(quarters):
        for front, piece in every_piece:
            product_copy(quarter, front, piece).wait_send()
            samples_copy(quarter, front, piece).wait_send()
        projected_copy(quarter).wait()


def pipeline(fronts, samples, second_samples, front_sizes, parent_ids, block_maps):
    local, height, depth = fronts.shape
    groups, cols = lax.axis_size("group"), lax.axis_size("col")
    block = second_samples.shape[0] // QUARTERS
    half = samples.shape[0] // QUARTERS
    first = samples.reshape(half // block, QUARTERS, block, local, depth)
    first = first.transpose(1, 3, 0, 2, 4).reshape(QUARTERS, local, half, depth)
    second = second_samples.reshape(QUARTERS, block, local, height).transpose(2, 0, 1, 3)
    def vmem(*shape, dtype=jnp.bfloat16):
        return pltpu.VMEM(shape, dtype)

    def sems(*shape):
        return pltpu.SemaphoreType.DMA(shape)

    in_smem = pl.BlockSpec(memory_space=pltpu.SMEM)
    anywhere = pl.BlockSpec(memory_space=pl.ANY)
    f32 = jnp.float32
    sampled, projected = pl.pallas_call(
        functools.partial(fused, cols, groups),
        out_shape=(
            jax.ShapeDtypeStruct((local, QUARTERS, block, height), jnp.bfloat16),
            jax.ShapeDtypeStruct((QUARTERS, local, half, depth), jnp.bfloat16),
        ),
        in_specs=[anywhere, anywhere, anywhere, in_smem, in_smem, in_smem],
        out_specs=(anywhere, anywhere),
        scratch_shapes=[
            vmem(local, QUARTERS, block, height),
            vmem(QUARTERS, local, 2 * half, depth),
            vmem(FRONT_SLOTS, local, TILE, depth),
            vmem(PARTIAL_SLOTS, cols, local, 2, block, TILE),
            vmem(OUT_SLOTS, cols, local, 2, block, TILE),
            vmem(IN_SLOTS, cols, local, 2, block, TILE),
            vmem(OUT_SLOTS, cols, local, 2, block, TILE),
            vmem(IN_SLOTS, cols, local, 2, block, TILE),
            vmem(SLOTS, 2, local, 2, block, TILE),
            vmem(SLOTS, groups, local, 2, block, TILE),
            vmem(GATHER_SLOTS, local, cols, 2, block, TILE),
            vmem(QUARTERS, local, 2 * half, depth, dtype=f32),
            vmem(QUARTERS, local, half, depth),
            sems(FRONT_SLOTS),
            sems(QUARTERS),
            pltpu.SemaphoreType.DMA,
            sems(SLOTS, 2),
            sems(QUARTERS),
            sems(QUARTERS, local, half // block),
            sems(QUARTERS, local, half // block),
            sems(QUARTERS, local, half // block),
            sems(QUARTERS, local, half // block),
            sems(OUT_SLOTS, cols),
            sems(IN_SLOTS, cols),
            sems(OUT_SLOTS, cols),
            sems(IN_SLOTS, cols),
            sems(SLOTS),
            sems(SLOTS),
            sems(SLOTS, groups),
            sems(SLOTS, groups),
            sems(GATHER_SLOTS, cols),
            sems(GATHER_SLOTS, cols),
            sems(GATHER_SLOTS, cols),
            sems(GATHER_SLOTS, cols),
        ],
        compiler_params=pltpu.CompilerParams(
            collective_id=0, has_side_effects=True, vmem_limit_bytes=67043328
        ),
    )(first, fronts, second, front_sizes, parent_ids, block_maps.T)
    sampled = sampled.transpose(1, 2, 0, 3).reshape(second_samples.shape)
    projected = projected.reshape(QUARTERS, local, half // block, block, depth)
    projected = projected.transpose(2, 0, 3, 1, 4).reshape(samples.shape)
    return sampled, projected


def fits(mesh, fronts, samples, second_samples, block_maps):
    rows, cols = mesh.shape["row"], mesh.shape["col"]
    height, depth = fronts.shape[1] // rows, fronts.shape[2] // cols
    block = second_samples.shape[0] // cols // QUARTERS
    return (
        rows == 2
        and cols == 4
        and block_maps.shape[1] == rows
        and height % TILE == 0
        and height // TILE >= 2 * EDGE_TILES
        and depth % 128 == 0
        and second_samples.shape[0] % (cols * QUARTERS) == 0
        and block % 16 == 0
    )


def solution(mesh):
    placed = (
        P("group", "row", "col"),
        P("row", "group", "col"),
        P("col", "group", "row"),
        P(),
        P(),
        P(),
    )

    def step(fronts, samples, second_samples, front_sizes, parent_ids, block_maps):
        fast = fits(mesh, fronts, samples, second_samples, block_maps)
        return jax.shard_map(
            pipeline if fast else shards,
            mesh=mesh,
            in_specs=placed,
            out_specs=(P("col", "group", "row"), P("row", "group", "col")),
            check_vma=False,
        )(fronts, samples, second_samples, front_sizes, parent_ids, block_maps)

    return step
```
